32 devices in a mesh: band: 16 (over z, y, core), ga: 2 (over x).
Axes of the slice: x: 2, y: 2, z: 4, core: 2. Of those that a mesh axis runs over, the one named last changes fastest.
Arguments:
- orbitals: bfloat16 [2, 16, 160, 128], P(None, 'band', 'ga'), may hold values from -8 to 8, as said below
- potential: float32 [480, 480], P('ga'), may hold values from -2 to 2
- slot_sticks: int32 [160], replicated, may hold values from -1 to 126, as said below
- stick_entries: int32 [160, 128], replicated, may hold values from -1 to 126, as said below
Outputs:
- applied_orbitals: bfloat16 [2, 16, 160, 128], P(None, 'band', 'ga')
- correlation: float32 [2, 16, 16], replicated
- reduced_hamiltonian: float32 [2, 16, 16], replicated
The draws below stay inside these ranges and needn't reach their ends.
Inputs may be any that keep to these rules, and one draw needn't show every extreme that they name: `slot_sticks`: every gx with |gx| < 64 is held by exactly one slot; the other slots hold -1. Slots t with t // 80 = d are those of index d of ga; on some index of ga all 80 slots hold sticks. `stick_entries`: row t lists, in some order, gz + 63 for every gz with gx^2 + gz^2 < 64^2, gx being the stick of slot t, then -1 to the end of the row; rows of empty slots are all -1. `orbitals`: entries where stick_entries is -1 carry values that are not used.
All inputs are finite; a program needn't handle non-finite values.
Results may differ from the reference program's by a relative error of at most 0.001.
Values may be sent and summed in bfloat16 or wider, within the bound.
A program may use at most 64 MiB of HBM per device.

```python
import jax
import jax.numpy as jnp
from jax import lax

NGRID = 480
RAD = 64
KMAX = 128
SLOTS = 80
SLOT_ALL = 160
NB = 16
N_GA = 2


def stick_layout(key):
    stick_count = 2 * RAD - 1
    key_device, key_picked, key_ordering = jax.random.split(jax.random.fold_in(key, 11), 3)
    full_device = jax.random.randint(key_device, (), 0, N_GA)
    slot_ids = jnp.arange(SLOT_ALL, dtype=jnp.int32)
    owners = slot_ids // SLOTS
    others = jnp.where(owners > full_device, slot_ids - SLOTS, slot_ids)
    picked = jax.random.permutation(key_picked, (N_GA - 1) * SLOTS).astype(jnp.int32)
    chosen = jnp.take(picked, jnp.clip(others, 0, (N_GA - 1) * SLOTS - 1)) < stick_count - SLOTS
    occupied = jnp.where(owners == full_device, True, chosen)
    ranking = jnp.cumsum(occupied.astype(jnp.int32)) - 1
    ordering = jax.random.permutation(key_ordering, stick_count).astype(jnp.int32)
    return jnp.where(occupied, jnp.take(ordering, jnp.clip(ranking, 0, stick_count - 1)), -1).astype(jnp.int32)


def draw_slot_sticks(key, part):
    return stick_layout(key)


def draw_stick_entries(key, part):
    sticks = stick_layout(key)
    gx_value = sticks - RAD + 1
    offsets = jnp.arange(RAD, dtype=jnp.int32)
    half_width = jnp.sum((offsets * offsets)[None, :] + (gx_value * gx_value)[:, None] < RAD * RAD, axis=1).astype(jnp.int32) - 1
    length = jnp.where(sticks >= 0, 2 * half_width + 1, 0)
    column_ids = jnp.arange(KMAX, dtype=jnp.int32)
    inside = column_ids[None, :] < length[:, None]
    positions = jnp.where(inside, RAD - 1 - half_width[:, None] + column_ids[None, :], -1)
    jitter = jax.random.randint(jax.random.fold_in(key, 23), (SLOT_ALL, KMAX), 0, 4096)
    scores = jnp.where(inside, jitter, 4096) * KMAX + column_ids[None, :]
    ordering = jnp.argsort(scores, axis=1)
    return jnp.take_along_axis(positions, ordering, axis=1).astype(jnp.int32)


def draw_orbitals(key, part):
    key_own, key_common, key_weight, key_flip = jax.random.split(jax.random.fold_in(key, 37), 4)
    private = jax.random.normal(key_own, (2, NB, SLOT_ALL, KMAX), jnp.float32)
    weight = jax.random.uniform(key_weight, (NB,), jnp.float32, 0.5, 1.5)
    common = jax.random.normal(key_common, (2, 1, SLOT_ALL, KMAX), jnp.float32)
    sign_flip = jnp.where(jax.random.bernoulli(key_flip, 0.5, (NB,)), 1.0, -1.0)
    values = private + (weight * sign_flip)[None, :, None, None] * common
    return jnp.clip(values, -8.0, 8.0).astype(jnp.bfloat16)


def steps_of(rng, shape, pieces, smallest, high):
    loudness, own = 1.0, jax.random.fold_in(rng, 6)
    for dim, parts in pieces:
        steps = jnp.exp(jax.random.uniform(jax.random.fold_in(own, dim), (parts,), jnp.float32, smallest / len(pieces), high / len(pieces)))
        loudness = loudness * jnp.repeat(steps, shape[dim] // parts).reshape([-1 if axis == dim else 1 for axis in range(len(shape))])
    return loudness


def setup_inputs(seed: int = 0) -> dict:
    key_of = jax.random.split(jax.random.key(seed), 5)
    return {
        "orbitals": draw_orbitals(jax.random.fold_in(key_of[4], 71), 0),
        "potential": jnp.clip(jax.random.uniform(key_of[1], (NGRID, NGRID), jnp.float32, -2.0, 2.0) * steps_of(key_of[1], (NGRID, NGRID), ((0, 2),), -0.4, 0.0), -2.0, 2.0),
        "slot_sticks": draw_slot_sticks(jax.random.fold_in(key_of[4], 71), 0),
        "stick_entries": draw_stick_entries(jax.random.fold_in(key_of[4], 71), 0),
    }


TWO_PI = 6.283185307179586
HIGHEST_PRECISION = lax.Precision.HIGHEST


def phases(frequency, position, points):
    winding = (frequency[:, None] * position[None, :]) % points
    angles = winding.astype(jnp.float32) * (TWO_PI / points)
    return jnp.cos(angles), jnp.sin(angles)


def stick_phases(slot_sticks, radius, points):
    frequency = slot_sticks - radius + 1
    x_cos, x_sin = phases(frequency, jnp.arange(points, dtype=jnp.int32), points)
    filled = (slot_sticks >= 0).astype(jnp.float32)[:, None]
    return x_cos * filled, x_sin * filled


def unpack(coeffs, entry_lists):
    slot_count, width = entry_lists.shape
    leading = coeffs.shape[:2]
    flat_index = jnp.where(entry_lists >= 0, entry_lists + width * jnp.arange(slot_count, dtype=jnp.int32)[:, None], slot_count * width)
    spread = jnp.zeros(leading + (slot_count * width,), jnp.float32)
    values = coeffs.reshape(leading + (slot_count * width,)).astype(jnp.float32)
    spread = spread.at[:, :, flat_index.reshape(-1)].add(values, mode="drop")
    return spread.reshape(coeffs.shape)


def z_forward(spread, z_cos, z_sin):
    real_part = jnp.einsum("bsp,pz->bsz", spread[0], z_cos, precision=HIGHEST_PRECISION) - jnp.einsum("bsp,pz->bsz", spread[1], z_sin, precision=HIGHEST_PRECISION)
    imag_part = jnp.einsum("bsp,pz->bsz", spread[0], z_sin, precision=HIGHEST_PRECISION) + jnp.einsum("bsp,pz->bsz", spread[1], z_cos, precision=HIGHEST_PRECISION)
    return jnp.stack([real_part, imag_part])


def plane_work(columns, x_cos, x_sin, potential):
    field_real = jnp.einsum("bsz,sx->bzx", columns[0], x_cos, precision=HIGHEST_PRECISION) - jnp.einsum("bsz,sx->bzx", columns[1], x_sin, precision=HIGHEST_PRECISION)
    field_imag = jnp.einsum("bsz,sx->bzx", columns[0], x_sin, precision=HIGHEST_PRECISION) + jnp.einsum("bsz,sx->bzx", columns[1], x_cos, precision=HIGHEST_PRECISION)
    prod_real = potential[None] * field_real
    prod_imag = potential[None] * field_imag
    back_real = jnp.einsum("bzx,sx->bsz", prod_real, x_cos, precision=HIGHEST_PRECISION) + jnp.einsum("bzx,sx->bsz", prod_imag, x_sin, precision=HIGHEST_PRECISION)
    back_imag = jnp.einsum("bzx,sx->bsz", prod_imag, x_cos, precision=HIGHEST_PRECISION) - jnp.einsum("bzx,sx->bsz", prod_real, x_sin, precision=HIGHEST_PRECISION)
    return jnp.stack([back_real, back_imag])


def z_backward(gathered, z_cos, z_sin, points):
    real_part = jnp.einsum("bsz,pz->bsp", gathered[0], z_cos, precision=HIGHEST_PRECISION) + jnp.einsum("bsz,pz->bsp", gathered[1], z_sin, precision=HIGHEST_PRECISION)
    imag_part = jnp.einsum("bsz,pz->bsp", gathered[1], z_cos, precision=HIGHEST_PRECISION) - jnp.einsum("bsz,pz->bsp", gathered[0], z_sin, precision=HIGHEST_PRECISION)
    return jnp.stack([real_part, imag_part]) / float(points * points)


def kinetic_factor(sticks, entry_lists, radius):
    gx_value = sticks - radius + 1
    gz_value = entry_lists - radius + 1
    return ((gx_value * gx_value)[:, None] + gz_value * gz_value).astype(jnp.float32) / float(radius * radius)


def cross_products(left, right, scale):
    dims = (((1,), (1,)), ((), ()))
    real_part = lax.dot_general(left[0], right[0], dims, preferred_element_type=jnp.float32) + lax.dot_general(left[1], right[1], dims, preferred_element_type=jnp.float32)
    imag_part = lax.dot_general(left[0], right[1], dims, preferred_element_type=jnp.float32) - lax.dot_general(left[1], right[0], dims, preferred_element_type=jnp.float32)
    return jnp.stack([real_part, imag_part]) * scale


def reference(orbitals, potential, slot_sticks, stick_entries):
    points = potential.shape[1]
    width = stick_entries.shape[1]
    radius = width // 2
    band_total = orbitals.shape[1]
    present = stick_entries >= 0
    masked = jnp.where(present[None, None], orbitals, jnp.zeros_like(orbitals))
    spread = unpack(orbitals, stick_entries)
    frequency = jnp.arange(width, dtype=jnp.int32) - radius + 1
    z_cos, z_sin = phases(frequency, jnp.arange(points, dtype=jnp.int32), points)
    x_cos, x_sin = stick_phases(slot_sticks, radius, points)

    def one_band(coeffs):
        columns = z_forward(coeffs[:, None], z_cos, z_sin)
        gathered = plane_work(columns, x_cos, x_sin, potential)
        return z_backward(gathered, z_cos, z_sin, points)[:, 0]

    spectra = jnp.moveaxis(lax.map(one_band, jnp.moveaxis(spread, 1, 0)), 0, 1)
    indices = jnp.broadcast_to(jnp.clip(stick_entries, 0, width - 1)[None, None], spectra.shape)
    applied = jnp.take_along_axis(spectra, indices, axis=3)
    kinetic = kinetic_factor(slot_sticks, stick_entries, radius)
    applied_orbitals = jnp.where(present[None, None], kinetic[None, None] * orbitals.astype(jnp.float32) + applied, jnp.float32(0.0)).astype(jnp.bfloat16)
    scale = 1.0 / (4.0 * radius * radius)
    flat_psi = masked.reshape(2, band_total, -1)
    flat_h = applied_orbitals.reshape(2, band_total, -1)
    correlation = cross_products(flat_psi, flat_psi, scale)
    reduced_hamiltonian = cross_products(flat_psi, flat_h, scale)
    return applied_orbitals, correlation, reduced_hamiltonian
```

```python
import functools
import math

import jax
import jax.numpy as jnp
import numpy as np
from jax import lax
from jax.experimental import pallas as pl
from jax.experimental.pallas import tpu as pltpu
from jax.sharding import PartitionSpec as P

MESH = pl.DeviceIdType.MESH
NT = (((1,), (1,)), ((), ()))
BF16 = jnp.bfloat16
F32 = jnp.float32
BLOCK = 4
UNROLL = 8


def split_np(table):
    high = table.astype(np.float32).astype(BF16)
    low = (table - high.astype(np.float64)).astype(np.float32).astype(BF16)
    return np.stack([high, low])


def tables(points, width, radius, groups, planes, plane_pad, coarse):
    freq = np.arange(width) - radius + 1
    used = (np.arange(width) < width - 1).astype(np.float64)
    z_tabs = []
    for group in range(groups):
        z = np.arange(planes) + group * planes
        angle = 2.0 * np.pi * ((freq[:, None] * z[None, :]) % points) / points
        cos = np.zeros((width, plane_pad))
        sin = np.zeros((width, plane_pad))
        cos[:, :planes] = np.cos(angle) * used[:, None]
        sin[:, :planes] = np.sin(angle) * used[:, None]
        z_tabs.append(split_np(np.block([[cos, sin], [-sin, cos]])))
    x = np.arange(coarse)
    angle = 2.0 * np.pi * ((freq[None, :] * x[:, None]) % coarse) / coarse
    cos = np.cos(angle) * used[None, :]
    sin = np.sin(angle) * used[None, :]
    forward = np.block([[cos, -sin], [sin, cos]])
    limit = 2 * (radius - 1)
    offset = (x[:, None] * points - np.arange(points)[None, :] * coarse) % (coarse * points)
    base = 2.0 * np.pi * offset / (coarse * points)
    resample = np.ones((coarse, points))
    for g in range(1, limit + 1):
        resample += 2.0 * np.cos(g * base)
    resample /= points
    return (
        np.stack(z_tabs),
        split_np(forward),
        split_np(forward.T.copy()),
        split_np(resample),
    )


def split(value):
    high = value.astype(BF16)
    low = (value - high.astype(F32)).astype(BF16)
    return high, low


def dot(a, b):
    return jnp.dot(a, b, preferred_element_type=F32)


def dot_nt(a, b):
    return lax.dot_general(a, b, NT, preferred_element_type=F32)


def take_lanes(value, index):
    return jnp.take_along_axis(value, index, axis=1, mode="promise_in_bounds")


def kernel(
    bands,
    groups,
    points,
    radius,
    orb_hbm,
    slots_hbm,
    entries_hbm,
    pot_hbm,
    tz_hbm,
    tx_hbm,
    ty_hbm,
    tr_hbm,
    out_ref,
    corr_ref,
    red_ref,
    orb_ref,
    slots_ref,
    entries_ref,
    tz,
    tx,
    ty,
    tr,
    pot,
    ent_t,
    inv_ref,
    raw,
    spread,
    colbuf,
    part,
    got,
    dense_ref,
    pdense,
    inbox_m,
    inbox_p,
    left_f,
    right_f,
    message,
    inbox_s,
    load_sem,
    near_sem,
    s_send,
    s_recv,
    x_send,
    x_recv,
    m_send,
    m_recv,
    p_send,
    p_recv,
    b_send,
    b_recv,
):
    band = lax.axis_index("band")
    ga = lax.axis_index("ga")
    total = bands * groups
    me = ga * bands + band
    slots = orb_hbm.shape[2]
    width = orb_hbm.shape[3]
    planes = pot_hbm.shape[0]
    plane_pad = pot.shape[0]
    coarse = ty.shape[2] // 2
    reducers = inbox_s.shape[0]
    rows = width // reducers
    per_group = reducers // groups
    block = math.gcd(bands, BLOCK)
    blocks = bands // block
    place = lax.rem(band, block)
    base = band - place
    first_band = bands // 2 - per_group + 1

    loads = [
        pltpu.make_async_copy(entries_hbm, entries_ref, load_sem.at[5]),
        pltpu.make_async_copy(orb_hbm, orb_ref, load_sem.at[6]),
        pltpu.make_async_copy(slots_hbm, slots_ref, load_sem.at[7]),
        pltpu.make_async_copy(pot_hbm, pot.at[pl.ds(0, planes)], load_sem.at[0]),
        pltpu.make_async_copy(tr_hbm, tr, load_sem.at[1]),
        pltpu.make_async_copy(tz_hbm.at[ga], tz, load_sem.at[2]),
        pltpu.make_async_copy(tx_hbm, tx, load_sem.at[3]),
        pltpu.make_async_copy(ty_hbm, ty, load_sem.at[4]),
    ]
    load_entries, load_orb, load_slots, load_pot, load_tr, load_tz, load_tx, load_ty = loads
    load_orb.start()

    has_low = band >= block
    has_high = band < bands - block
    barrier = pltpu.get_barrier_semaphore()
    for g in range(groups):
        for c in range(block):
            if g or c:
                pl.semaphore_signal(
                    barrier,
                    inc=1,
                    device_id=(base + lax.rem(place + c, block), lax.rem(ga + g, groups)),
                    device_id_type=MESH,
                )

    def near(semaphore_low, semaphore_high):
        @pl.when(has_low)
        def _():
            pl.semaphore_signal(
                semaphore_high, inc=1, device_id=(band - block, ga), device_id_type=MESH
            )

        @pl.when(has_high)
        def _():
            pl.semaphore_signal(
                semaphore_low, inc=1, device_id=(band + block, ga), device_id_type=MESH
            )

    def near_wait():
        @pl.when(has_low)
        def _():
            pl.semaphore_wait(near_sem.at[0], 1)

        @pl.when(has_high)
        def _():
            pl.semaphore_wait(near_sem.at[1], 1)

    near(barrier, barrier)
    for load in loads:
        if load is not load_orb:
            load.start()
    if plane_pad > planes:
        pot[pl.ds(planes, plane_pad - planes), :] = jnp.zeros(
            (plane_pad - planes, pot.shape[1]), F32
        )

    load_orb.wait()
    pl.semaphore_wait(
        barrier, block * groups - 1 + has_low.astype(jnp.int32) + has_high.astype(jnp.int32)
    )
    s_copies = []
    for k in range(1, groups):
        copy = pltpu.make_async_remote_copy(
            src_ref=orb_ref.at[:, 0],
            dst_ref=raw.at[k - 1],
            send_sem=s_send.at[k - 1],
            recv_sem=s_recv.at[k - 1],
            device_id=(band, lax.rem(ga + k, groups)),
            device_id_type=MESH,
        )
        copy.start()
        s_copies.append(copy)
    near(near_sem.at[0], near_sem.at[1])

    load_entries.wait()
    load_slots.wait()
    all_slots = groups * slots
    listed = entries_ref[...].astype(F32)
    slot_pad = ent_t.shape[1] - all_slots
    if slot_pad:
        listed = jnp.concatenate([listed, jnp.full((slot_pad, width), -1.0, F32)], axis=0)
    ent_t[...] = listed.T
    lanes = ent_t.shape[1]
    which = lax.broadcasted_iota(jnp.int32, (width, lanes), 0).astype(F32).astype(BF16)

    def invert(step, found):
        for u in range(UNROLL):
            k = step * UNROLL + u
            row = jnp.broadcast_to(ent_t[pl.ds(k, 1), :], (16, lanes)).astype(BF16)
            row = jnp.concatenate([row] * (width // 16), axis=0)
            found = jnp.where(row == which, k.astype(F32).astype(BF16), found)
        return found

    found = lax.fori_loop(
        0, width // UNROLL, invert, jnp.full((width, lanes), -1.0, BF16)
    )
    found = found.astype(F32).T.astype(jnp.int32)
    for g in range(groups):
        inv_ref[g] = found[g * slots : (g + 1) * slots]

    def spread_of(g, re, im):
        inverse = inv_ref[g]
        filled = inverse >= 0
        index = jnp.maximum(inverse, 0)
        spread[g, :, :width] = jnp.where(filled, take_lanes(re, index), 0.0).astype(BF16)
        spread[g, :, width:] = jnp.where(filled, take_lanes(im, index), 0.0).astype(BF16)

    re = orb_ref[0, 0].astype(F32)
    im = orb_ref[1, 0].astype(F32)
    spread_of(ga, re, im)

    near_wait()
    rounds = max(blocks // 2, 1)
    if rounds > 1:
        near(near_sem.at[0], near_sem.at[1])

    load_pot.wait()
    load_tr.wait()
    pot_hi, pot_lo = split(pot[...])
    weight = dot_nt(tr[0], pot_hi) + dot_nt(tr[0], pot_lo) + dot_nt(tr[1], pot_hi)

    for k, copy in enumerate(s_copies, 1):
        copy.wait()
        spread_of(
            lax.rem(ga - k + groups, groups), raw[k - 1, 0].astype(F32), raw[k - 1, 1].astype(F32)
        )
    all_sticks = slots_ref[...].reshape(1, all_slots)
    sticks = [all_sticks[:, g * slots : (g + 1) * slots] for g in range(groups)]
    dense = jnp.zeros((width, 2 * width), F32)
    sub = lax.broadcasted_iota(jnp.int32, (width, slots), 0)
    for g in range(groups):
        choose = jnp.where(sub == sticks[g], 1.0, 0.0).astype(BF16)
        dense += dot(choose, spread[g])
    dense = dense.astype(BF16)
    dense_ref[...] = dense

    for r in range(1, rounds):
        near_wait()
        if r < rounds - 1:
            near(near_sem.at[0], near_sem.at[1])

    def place_of(r):
        return first_band + 2 * (r % per_group), r // per_group

    def m_copy(q):
        start = pl.multiple_of((ga * per_group + q) * rows, rows)
        return pltpu.make_async_remote_copy(
            src_ref=dense_ref.at[pl.ds(start, rows)],
            dst_ref=inbox_m.at[band],
            send_sem=m_send.at[q],
            recv_sem=m_recv,
            device_id=(first_band + 2 * q, ga),
            device_id_type=MESH,
        )

    def m_each(act, own):
        for q in range(per_group):
            mine = band == first_band + 2 * q

            @pl.when(jnp.logical_not(mine))
            def _(q=q):
                act(m_copy(q))

            if own:

                @pl.when(mine)
                def _(q=q):
                    start = pl.multiple_of((ga * per_group + q) * rows, rows)
                    inbox_m[band] = dense_ref[pl.ds(start, rows), :]

    m_each(lambda copy: copy.start(), True)

    load_tz.wait()
    columns = dot(dense, tz[0]) + dot(dense, tz[1])
    col_hi, col_lo = split(columns)
    colbuf[0, :width] = col_hi[:, :plane_pad]
    colbuf[0, width:] = col_hi[:, plane_pad:]
    colbuf[1, :width] = col_lo[:, :plane_pad]
    colbuf[1, width:] = col_lo[:, plane_pad:]
    load_tx.wait()
    field = dot(tx[0], colbuf[0]) + dot(tx[0], colbuf[1]) + dot(tx[1], colbuf[0])
    product = jnp.concatenate([field[:coarse] * weight, field[coarse:] * weight], axis=0)
    pro_hi, pro_lo = split(product)
    load_ty.wait()
    back = dot(ty[0], pro_hi) + dot(ty[0], pro_lo) + dot(ty[1], pro_hi)
    back = jnp.concatenate([back[:width], back[width:]], axis=1)
    back_hi, back_lo = split(back)
    spectra = dot_nt(back_hi, tz[0]) + dot_nt(back_hi, tz[1]) + dot_nt(back_lo, tz[0])
    spectra = spectra * (1.0 / float(points * coarse))
    spec_hi, spec_lo = split(spectra)
    pdense[...] = spec_hi

    def p_copy(r):
        return pltpu.make_async_remote_copy(
            src_ref=pdense.at[pl.ds(r * rows, rows)],
            dst_ref=inbox_p.at[me],
            send_sem=p_send.at[r],
            recv_sem=p_recv,
            device_id=place_of(r),
            device_id_type=MESH,
        )

    def p_each(act, own):
        for r in range(reducers):
            to_band, to_ga = place_of(r)
            mine = me == to_ga * bands + to_band

            @pl.when(jnp.logical_not(mine))
            def _(r=r):
                act(p_copy(r))

            if own:

                @pl.when(mine)
                def _(r=r):
                    inbox_p[me] = pdense[pl.ds(r * rows, rows), :]

    p_each(lambda copy: copy.start(), True)

    eye = lax.broadcasted_iota(jnp.int32, (slots, slots), 0) == lax.broadcasted_iota(
        jnp.int32, (slots, slots), 1
    )

    def stick_column(g):
        row = sticks[0]
        for other in range(1, groups):
            row = jnp.where(g == other, sticks[other], row)
        row = row.astype(F32)
        return jnp.sum(jnp.where(eye, row, 0.0), axis=1, keepdims=True)

    lane = lax.broadcasted_iota(jnp.int32, (slots, width), 1)
    lane_f = lane.astype(F32)
    x_copies = []
    for k in range(1, groups + 1):
        target = lax.rem(ga + k, groups)
        stick = stick_column(target)
        choose = jnp.where(stick == lane_f, 1.0, 0.0).astype(BF16)
        mine = dot(choose, spec_hi) + dot(choose, spec_lo)
        if k < groups:
            part[k - 1] = mine
            copy = pltpu.make_async_remote_copy(
                src_ref=part.at[k - 1],
                dst_ref=got.at[k - 1],
                send_sem=x_send.at[k - 1],
                recv_sem=x_recv.at[k - 1],
                device_id=(band, target),
                device_id_type=MESH,
            )
            copy.start()
            x_copies.append(copy)

    own = entries_ref[pl.ds(pl.multiple_of(ga * slots, 8), slots)]
    present = own >= 0
    gx = stick - float(radius - 1)
    gz = (own - (radius - 1)).astype(F32)
    kinetic = (gx * gx + gz * gz) * (1.0 / float(radius * radius))
    own_index = jnp.maximum(own, 0)

    for copy in x_copies:
        copy.wait()
    for k in range(1, groups):
        mine += got[k - 1]
    a_re = take_lanes(mine[:, :width], own_index)
    a_im = take_lanes(mine[:, width:], own_index)
    out_ref[0, 0] = jnp.where(present, kinetic * re + a_re, 0.0).astype(BF16)
    out_ref[1, 0] = jnp.where(present, kinetic * im + a_im, 0.0).astype(BF16)

    offset = band - first_band
    is_reducer = (offset >= 0) & (offset < 2 * per_group) & (lax.rem(offset + 2 * bands, 2) == 0)
    number = ga * per_group + lax.div(jnp.clip(offset, 0, 2 * per_group - 1), 2)

    def b_copy(t):
        return pltpu.make_async_remote_copy(
            src_ref=message,
            dst_ref=inbox_s.at[number],
            send_sem=b_send.at[t],
            recv_sem=b_recv,
            device_id=(t // groups, t % groups) if isinstance(t, int) else (lax.div(t, groups), lax.rem(t, groups)),
            device_id_type=MESH,
        )

    def b_each(act):
        order = band * groups + ga
        if total <= 64:
            for t in range(total):

                @pl.when(order != t)
                def _(t=t):
                    act(b_copy(t))
        else:

            @pl.loop(0, total)
            def _(t):
                @pl.when(order != t)
                def _():
                    act(b_copy(t))

    @pl.when(is_reducer)
    def _():
        m_all = inbox_m.at[pl.ds(0, bands - 1)]
        pltpu.make_async_copy(m_all, m_all, m_recv).wait()
        left = inbox_m[...].astype(F32)
        for c in range(2):
            left_f[c] = left[:, :, c * width : (c + 1) * width].reshape(bands * rows, width)
        row_id = lax.broadcasted_iota(jnp.int32, (rows, 2 * width), 0) + number * rows
        lane_id = lax.broadcasted_iota(jnp.int32, (rows, 2 * width), 1)
        row_f = (row_id - (radius - 1)).astype(F32)
        lane_g = (jnp.where(lane_id >= width, lane_id - width, lane_id) - (radius - 1)).astype(F32)
        kin = (row_f * row_f + lane_g * lane_g) * (1.0 / float(radius * radius))
        right = left * kin[None]
        p_all = inbox_p.at[pl.ds(0, total - 1)]
        pltpu.make_async_copy(p_all, p_all, p_recv).wait()
        for g in range(groups):
            right += inbox_p[g * bands : (g + 1) * bands].astype(F32)
        for c in range(2):
            right_f[c] = right[:, :, c * width : (c + 1) * width].reshape(bands * rows, width)
        result = jnp.zeros((bands, 4 * bands), F32)
        for r in range(rows):
            every = pl.ds(r, bands, stride=rows)
            low_re, low_im = left_f[0, every, :], left_f[1, every, :]
            high_re, high_im = right_f[0, every, :], right_f[1, every, :]
            low = jnp.concatenate([low_re, low_im], axis=1)
            stack = jnp.concatenate(
                [
                    jnp.concatenate([high_re, high_im], axis=1),
                    jnp.concatenate([high_im, -high_re], axis=1),
                    low,
                    jnp.concatenate([low_im, -low_re], axis=1),
                ],
                axis=0,
            )
            result += dot_nt(low.astype(BF16), stack.astype(BF16))
        result = result * (1.0 / float(4 * radius * radius))
        fold = message.shape[1] // (4 * bands)
        depth = message.shape[0]
        message[...] = jnp.concatenate(
            [result[f * depth : (f + 1) * depth] for f in range(fold)], axis=1
        )
        inbox_s[number] = message[...]
        b_each(lambda copy: copy.start())
        most = inbox_s.at[pl.ds(0, reducers - 1)]
        pltpu.make_async_copy(most, most, b_recv).wait()

    @pl.when(jnp.logical_not(is_reducer))
    def _():
        pltpu.make_async_copy(inbox_s, inbox_s, b_recv).wait()

    final = inbox_s[0]
    for r in range(1, reducers):
        final += inbox_s[r]
    span = 4 * bands
    fold = message.shape[1] // span
    final = jnp.concatenate([final[:, f * span : (f + 1) * span] for f in range(fold)], axis=0)
    red_ref[0] = final[:, :bands]
    red_ref[1] = final[:, bands : 2 * bands]
    corr_ref[0] = final[:, 2 * bands : 3 * bands]
    corr_ref[1] = final[:, 3 * bands :]

    m_each(lambda copy: copy.wait_send(), False)
    p_each(lambda copy: copy.wait_send(), False)

    @pl.when(is_reducer)
    def _():
        b_each(lambda copy: copy.wait_send())


def write_out(out_ref, corr_ref, red_ref, out_hbm, corr_hbm, red_hbm, sem):
    copies = [
        pltpu.make_async_copy(out_ref, out_hbm, sem.at[0]),
        pltpu.make_async_copy(corr_ref, corr_hbm, sem.at[1]),
        pltpu.make_async_copy(red_ref, red_hbm, sem.at[2]),
    ]
    for copy in copies:
        copy.start()
    for copy in copies:
        copy.wait()


def body(bands, groups, orbitals, potential, slot_sticks, stick_entries):
    points = potential.shape[1]
    planes = potential.shape[0]
    width = stick_entries.shape[1]
    radius = width // 2
    slots = orbitals.shape[2]
    plane_pad = -(-planes // 128) * 128
    coarse = 2 * width
    reducers = width // 16
    per_group = reducers // groups
    rows = width // reducers
    fold = max(1, 128 // (4 * bands))
    slot_lanes = -(-groups * slots // 128) * 128
    tz, tx, ty, tr = tables(points, width, radius, groups, planes, plane_pad, coarse)
    vmem = pl.BlockSpec(memory_space=pltpu.VMEM)
    hbm = pl.BlockSpec(memory_space=pltpu.HBM)
    total = bands * groups
    dma = pltpu.SemaphoreType.DMA
    results = pl.pallas_call(
        functools.partial(kernel, bands, groups, points, radius),
        out_shape=(
            pltpu.VMEM(orbitals.shape, BF16),
            pltpu.VMEM((2, bands, bands), F32),
            pltpu.VMEM((2, bands, bands), F32),
        ),
        in_specs=[hbm] * 8,
        out_specs=(vmem, vmem, vmem),
        scratch_shapes=[
            pltpu.VMEM(orbitals.shape, BF16),
            pltpu.VMEM(slot_sticks.shape, jnp.int32),
            pltpu.VMEM(stick_entries.shape, jnp.int32),
            pltpu.VMEM(tz.shape[1:], BF16),
            pltpu.VMEM(tx.shape, BF16),
            pltpu.VMEM(ty.shape, BF16),
            pltpu.VMEM(tr.shape, BF16),
            pltpu.VMEM((plane_pad, points), F32),
            pltpu.VMEM((width, slot_lanes), F32),
            pltpu.VMEM((groups, slots, width), jnp.int32),
            pltpu.VMEM((groups - 1, 2, slots, width), BF16),
            pltpu.VMEM((groups, slots, 2 * width), BF16),
            pltpu.VMEM((2, 2 * width, plane_pad), BF16),
            pltpu.VMEM((groups - 1, slots, 2 * width), F32),
            pltpu.VMEM((groups - 1, slots, 2 * width), F32),
            pltpu.VMEM((width, 2 * width), BF16),
            pltpu.VMEM((width, 2 * width), BF16),
            pltpu.VMEM((bands, rows, 2 * width), BF16),
            pltpu.VMEM((total, rows, 2 * width), BF16),
            pltpu.VMEM((2, bands * rows, width), F32),
            pltpu.VMEM((2, bands * rows, width), F32),
            pltpu.VMEM((bands // fold, 4 * bands * fold), F32),
            pltpu.VMEM((reducers, bands // fold, 4 * bands * fold), F32),
            dma((8,)),
            pltpu.SemaphoreType.REGULAR((2,)),
            dma((groups - 1,)),
            dma((groups - 1,)),
            dma((groups - 1,)),
            dma((groups - 1,)),
            dma((per_group,)),
            dma,
            dma((reducers,)),
            dma,
            dma((total,)),
            dma,
        ],
        compiler_params=pltpu.CompilerParams(
            collective_id=0, has_side_effects=True, vmem_limit_bytes=60000000
        ),
    )(orbitals, slot_sticks, stick_entries, potential, tz, tx, ty, tr)
    return pl.pallas_call(
        write_out,
        out_shape=[jax.ShapeDtypeStruct(r.shape, r.dtype) for r in results],
        in_specs=[vmem] * 3,
        out_specs=[hbm] * 3,
        scratch_shapes=[dma((3,))],
    )(*results)


def solution(mesh):
    bands = mesh.shape["band"]
    groups = mesh.shape["ga"]
    return jax.shard_map(
        functools.partial(body, bands, groups),
        mesh=mesh,
        in_specs=(P(None, "band", "ga", None), P("ga", None), P(), P()),
        out_specs=(P(None, "band", "ga", None), P(), P()),
        check_vma=False,
    )
```

```python
import functools
import math

import jax
import jax.numpy as jnp
import numpy as np
from jax import lax
from jax.experimental import pallas as pl
from jax.experimental.pallas import tpu as pltpu
from jax.sharding import PartitionSpec as P

MESH = pl.DeviceIdType.MESH
NT = (((1,), (1,)), ((), ()))
BF16 = jnp.bfloat16
F32 = jnp.float32
BLOCK = 4
UNROLL = 8


def split_np(table):
    high = table.astype(np.float32).astype(BF16)
    low = (table - high.astype(np.float64)).astype(np.float32).astype(BF16)
    return np.stack([high, low])


def tables(points, width, radius, groups, planes, plane_pad, coarse):
    freq = np.arange(width) - radius + 1
    used = (np.arange(width) < width - 1).astype(np.float64)
    z_tabs = []
    for group in range(groups):
        z = np.arange(planes) + group * planes
        angle = 2.0 * np.pi * ((freq[:, None] * z[None, :]) % points) / points
        cos = np.zeros((width, plane_pad))
        sin = np.zeros((width, plane_pad))
        cos[:, :planes] = np.cos(angle) * used[:, None]
        sin[:, :planes] = np.sin(angle) * used[:, None]
        z_tabs.append(split_np(np.block([[cos, sin], [-sin, cos]])))
    x = np.arange(coarse)
    angle = 2.0 * np.pi * ((freq[None, :] * x[:, None]) % coarse) / coarse
    cos = np.cos(angle) * used[None, :]
    sin = np.sin(angle) * used[None, :]
    forward = np.block([[cos, -sin], [sin, cos]])
    limit = 2 * (radius - 1)
    offset = (x[:, None] * points - np.arange(points)[None, :] * coarse) % (coarse * points)
    base = 2.0 * np.pi * offset / (coarse * points)
    resample = np.ones((coarse, points))
    for g in range(1, limit + 1):
        resample += 2.0 * np.cos(g * base)
    resample /= points
    return (
        np.stack(z_tabs),
        split_np(forward),
        split_np(forward.T.copy()),
        split_np(resample),
    )


def split(value):
    high = value.astype(BF16)
    low = (value - high.astype(F32)).astype(BF16)
    return high, low


def dot(a, b):
    return jnp.dot(a, b, preferred_element_type=F32)


def dot_nt(a, b):
    return lax.dot_general(a, b, NT, preferred_element_type=F32)


def take_lanes(value, index):
    return jnp.take_along_axis(value, index, axis=1, mode="promise_in_bounds")


def kernel(
    bands,
    groups,
    points,
    radius,
    orb_hbm,
    slots_hbm,
    entries_hbm,
    pot_hbm,
    tz_hbm,
    tx_hbm,
    ty_hbm,
    tr_hbm,
    out_ref,
    corr_ref,
    red_ref,
    orb_ref,
    slots_ref,
    entries_ref,
    tz,
    tx,
    ty,
    tr,
    pot,
    ent_t,
    inv_ref,
    raw,
    spread,
    colbuf,
    part,
    got,
    dense_ref,
    pdense,
    inbox_m,
    inbox_p,
    left_f,
    right_f,
    message,
    inbox_s,
    load_sem,
    near_sem,
    s_send,
    s_recv,
    x_send,
    x_recv,
    m_send,
    m_recv,
    p_send,
    p_recv,
    b_send,
    b_recv,
):
    band = lax.axis_index("band")
    ga = lax.axis_index("ga")
    total = bands * groups
    me = ga * bands + band
    slots = orb_hbm.shape[2]
    width = orb_hbm.shape[3]
    planes = pot_hbm.shape[0]
    plane_pad = pot.shape[0]
    coarse = ty.shape[2] // 2
    reducers = inbox_s.shape[0]
    rows = width // reducers
    per_group = reducers // groups
    block = math.gcd(bands, BLOCK)
    blocks = bands // block
    place = lax.rem(band, block)
    base = band - place
    first_band = bands // 2 - per_group + 1

    loads = [
        pltpu.make_async_copy(entries_hbm, entries_ref, load_sem.at[5]),
        pltpu.make_async_copy(orb_hbm, orb_ref, load_sem.at[6]),
        pltpu.make_async_copy(slots_hbm, slots_ref, load_sem.at[7]),
        pltpu.make_async_copy(pot_hbm, pot.at[pl.ds(0, planes)], load_sem.at[0]),
        pltpu.make_async_copy(tr_hbm, tr, load_sem.at[1]),
        pltpu.make_async_copy(tz_hbm.at[ga], tz, load_sem.at[2]),
        pltpu.make_async_copy(tx_hbm, tx, load_sem.at[3]),
        pltpu.make_async_copy(ty_hbm, ty, load_sem.at[4]),
    ]
    load_entries, load_orb, load_slots, load_pot, load_tr, load_tz, load_tx, load_ty = loads
    load_orb.start()

    has_low = band >= block
    has_high = band < bands - block
    barrier = pltpu.get_barrier_semaphore()
    for g in range(groups):
        for c in range(block):
            if g or c:
                pl.semaphore_signal(
                    barrier,
                    inc=1,
                    device_id=(base + lax.rem(place + c, block), lax.rem(ga + g, groups)),
                    device_id_type=MESH,
                )

    def near(semaphore_low, semaphore_high):
        @pl.when(has_low)
        def _():
            pl.semaphore_signal(
                semaphore_high, inc=1, device_id=(band - block, ga), device_id_type=MESH
            )

        @pl.when(has_high)
        def _():
            pl.semaphore_signal(
                semaphore_low, inc=1, device_id=(band + block, ga), device_id_type=MESH
            )

    def near_wait():
        @pl.when(has_low)
        def _():
            pl.semaphore_wait(near_sem.at[0], 1)

        @pl.when(has_high)
        def _():
            pl.semaphore_wait(near_sem.at[1], 1)

    near(barrier, barrier)
    for load in loads:
        if load is not load_orb:
            load.start()
    if plane_pad > planes:
        pot[pl.ds(planes, plane_pad - planes), :] = jnp.zeros(
            (plane_pad - planes, pot.shape[1]), F32
        )

    load_orb.wait()
    pl.semaphore_wait(
        barrier, block * groups - 1 + has_low.astype(jnp.int32) + has_high.astype(jnp.int32)
    )
    s_copies = []
    for k in range(1, groups):
        copy = pltpu.make_async_remote_copy(
            src_ref=orb_ref.at[:, 0],
            dst_ref=raw.at[k - 1],
            send_sem=s_send.at[k - 1],
            recv_sem=s_recv.at[k - 1],
            device_id=(band, lax.rem(ga + k, groups)),
            device_id_type=MESH,
        )
        copy.start()
        s_copies.append(copy)
    near(near_sem.at[0], near_sem.at[1])

    load_entries.wait()
    load_slots.wait()
    all_slots = groups * slots
    listed = entries_ref[...].astype(F32)
    slot_pad = ent_t.shape[1] - all_slots
    if slot_pad:
        listed = jnp.concatenate([listed, jnp.full((slot_pad, width), -1.0, F32)], axis=0)
    ent_t[...] = listed.T
    lanes = ent_t.shape[1]
    which = lax.broadcasted_iota(jnp.int32, (width, lanes), 0).astype(F32).astype(BF16)

    def invert(step, found):
        for u in range(UNROLL):
            k = step * UNROLL + u
            row = jnp.broadcast_to(ent_t[pl.ds(k, 1), :], (16, lanes)).astype(BF16)
            row = jnp.concatenate([row] * (width // 16), axis=0)
            found = jnp.where(row == which, k.astype(F32).astype(BF16), found)
        return found

    found = lax.fori_loop(
        0, width // UNROLL, invert, jnp.full((width, lanes), -1.0, BF16)
    )
    found = found.astype(F32).T.astype(jnp.int32)
    for g in range(groups):
        inv_ref[g] = found[g * slots : (g + 1) * slots]

    def spread_of(g, re, im):
        inverse = inv_ref[g]
        filled = inverse >= 0
        index = jnp.maximum(inverse, 0)
        spread[g, :, :width] = jnp.where(filled, take_lanes(re, index), 0.0).astype(BF16)
        spread[g, :, width:] = jnp.where(filled, take_lanes(im, index), 0.0).astype(BF16)

    re = orb_ref[0, 0].astype(F32)
    im = orb_ref[1, 0].astype(F32)
    spread_of(ga, re, im)

    near_wait()
    rounds = max(blocks // 2, 1)
    if rounds > 1:
        near(near_sem.at[0], near_sem.at[1])

    load_pot.wait()
    load_tr.wait()
    pot_hi, pot_lo = split(pot[...])
    weight = dot_nt(tr[0], pot_hi) + dot_nt(tr[0], pot_lo) + dot_nt(tr[1], pot_hi)

    for k, copy in enumerate(s_copies, 1):
        copy.wait()
        spread_of(
            lax.rem(ga - k + groups, groups), raw[k - 1, 0].astype(F32), raw[k - 1, 1].astype(F32)
        )
    all_sticks = slots_ref[...].reshape(1, all_slots)
    sticks = [all_sticks[:, g * slots : (g + 1) * slots] for g in range(groups)]
    dense = jnp.zeros((width, 2 * width), F32)
    sub = lax.broadcasted_iota(jnp.int32, (width, slots), 0)
    for g in range(groups):
        choose = jnp.where(sub == sticks[g], 1.0, 0.0).astype(BF16)
        dense += dot(choose, spread[g])
    dense = dense.astype(BF16)
    dense_ref[...] = dense

    for r in range(1, rounds):
        near_wait()
        if r < rounds - 1:
            near(near_sem.at[0], near_sem.at[1])

    def place_of(r):
        return first_band + 2 * (r % per_group), r // per_group

    def m_copy(q):
        start = pl.multiple_of((ga * per_group + q) * rows, rows)
        return pltpu.make_async_remote_copy(
            src_ref=dense_ref.at[pl.ds(start, rows)],
            dst_ref=inbox_m.at[band],
            send_sem=m_send.at[q],
            recv_sem=m_recv,
            device_id=(first_band + 2 * q, ga),
            device_id_type=MESH,
        )

    def m_each(act, own):
        for q in range(per_group):
            mine = band == first_band + 2 * q

            @pl.when(jnp.logical_not(mine))
            def _(q=q):
                act(m_copy(q))

            if own:

                @pl.when(mine)
                def _(q=q):
                    start = pl.multiple_of((ga * per_group + q) * rows, rows)
                    inbox_m[band] = dense_ref[pl.ds(start, rows), :]

    m_each(lambda copy: copy.start(), True)

    load_tz.wait()
    columns = dot(dense, tz[0]) + dot(dense, tz[1])
    col_hi, col_lo = split(columns)
    colbuf[0, :width] = col_hi[:, :plane_pad]
    colbuf[0, width:] = col_hi[:, plane_pad:]
    colbuf[1, :width] = col_lo[:, :plane_pad]
    colbuf[1, width:] = col_lo[:, plane_pad:]
    load_tx.wait()
    field = dot(tx[0], colbuf[0]) + dot(tx[0], colbuf[1]) + dot(tx[1], colbuf[0])
    product = jnp.concatenate([field[:coarse] * weight, field[coarse:] * weight], axis=0)
    pro_hi, pro_lo = split(product)
    load_ty.wait()
    back = dot(ty[0], pro_hi) + dot(ty[0], pro_lo) + dot(ty[1], pro_hi)
    back = jnp.concatenate([back[:width], back[width:]], axis=1)
    back_hi, back_lo = split(back)
    spectra = dot_nt(back_hi, tz[0]) + dot_nt(back_hi, tz[1]) + dot_nt(back_lo, tz[0])
    spectra = spectra * (1.0 / float(points * coarse))
    spec_hi, spec_lo = split(spectra)
    pdense[...] = spec_hi

    def p_copy(r):
        return pltpu.make_async_remote_copy(
            src_ref=pdense.at[pl.ds(r * rows, rows)],
            dst_ref=inbox_p.at[me],
            send_sem=p_send.at[r],
            recv_sem=p_recv,
            device_id=place_of(r),
            device_id_type=MESH,
        )

    def p_each(act, own):
        for r in range(reducers):
            to_band, to_ga = place_of(r)
            mine = me == to_ga * bands + to_band

            @pl.when(jnp.logical_not(mine))
            def _(r=r):
                act(p_copy(r))

            if own:

                @pl.when(mine)
                def _(r=r):
                    inbox_p[me] = pdense[pl.ds(r * rows, rows), :]

    p_each(lambda copy: copy.start(), True)

    eye = lax.broadcasted_iota(jnp.int32, (slots, slots), 0) == lax.broadcasted_iota(
        jnp.int32, (slots, slots), 1
    )

    def stick_column(g):
        row = sticks[0]
        for other in range(1, groups):
            row = jnp.where(g == other, sticks[other], row)
        row = row.astype(F32)
        return jnp.sum(jnp.where(eye, row, 0.0), axis=1, keepdims=True)

    lane = lax.broadcasted_iota(jnp.int32, (slots, width), 1)
    lane_f = lane.astype(F32)
    x_copies = []
    for k in range(1, groups + 1):
        target = lax.rem(ga + k, groups)
        stick = stick_column(target)
        choose = jnp.where(stick == lane_f, 1.0, 0.0).astype(BF16)
        mine = dot(choose, spec_hi) + dot(choose, spec_lo)
        if k < groups:
            part[k - 1] = mine
            copy = pltpu.make_async_remote_copy(
                src_ref=part.at[k - 1],
                dst_ref=got.at[k - 1],
                send_sem=x_send.at[k - 1],
                recv_sem=x_recv.at[k - 1],
                device_id=(band, target),
                device_id_type=MESH,
            )
            copy.start()
            x_copies.append(copy)

    own = entries_ref[pl.ds(pl.multiple_of(ga * slots, 8), slots)]
    present = own >= 0
    gx = stick - float(radius - 1)
    gz = (own - (radius - 1)).astype(F32)
    kinetic = (gx * gx + gz * gz) * (1.0 / float(radius * radius))
    own_index = jnp.maximum(own, 0)

    for copy in x_copies:
        copy.wait()
    for k in range(1, groups):
        mine += got[k - 1]
    a_re = take_lanes(mine[:, :width], own_index)
    a_im = take_lanes(mine[:, width:], own_index)
    out_ref[0, 0] = jnp.where(present, kinetic * re + a_re, 0.0).astype(BF16)
    out_ref[1, 0] = jnp.where(present, kinetic * im + a_im, 0.0).astype(BF16)

    offset = band - first_band
    is_reducer = (offset >= 0) & (offset < 2 * per_group) & (lax.rem(offset + 2 * bands, 2) == 0)
    number = ga * per_group + lax.div(jnp.clip(offset, 0, 2 * per_group - 1), 2)

    def b_copy(t):
        return pltpu.make_async_remote_copy(
            src_ref=message,
            dst_ref=inbox_s.at[number],
            send_sem=b_send.at[t],
            recv_sem=b_recv,
            device_id=(t // groups, t % groups) if isinstance(t, int) else (lax.div(t, groups), lax.rem(t, groups)),
            device_id_type=MESH,
        )

    def b_each(act):
        order = band * groups + ga
        if total <= 64:
            for t in range(total):

                @pl.when(order != t)
                def _(t=t):
                    act(b_copy(t))
        else:

            @pl.loop(0, total)
            def _(t):
                @pl.when(order != t)
                def _():
                    act(b_copy(t))

    @pl.when(is_reducer)
    def _():
        m_all = inbox_m.at[pl.ds(0, bands - 1)]
        pltpu.make_async_copy(m_all, m_all, m_recv).wait()
        left = inbox_m[...].astype(F32)
        for c in range(2):
            left_f[c] = left[:, :, c * width : (c + 1) * width].reshape(bands * rows, width)
        row_id = lax.broadcasted_iota(jnp.int32, (rows, 2 * width), 0) + number * rows
        lane_id = lax.broadcasted_iota(jnp.int32, (rows, 2 * width), 1)
        row_f = (row_id - (radius - 1)).astype(F32)
        lane_g = (jnp.where(lane_id >= width, lane_id - width, lane_id) - (radius - 1)).astype(F32)
        kin = (row_f * row_f + lane_g * lane_g) * (1.0 / float(radius * radius))
        right = left * kin[None]
        p_all = inbox_p.at[pl.ds(0, total - 1)]
        pltpu.make_async_copy(p_all, p_all, p_recv).wait()
        for g in range(groups):
            right += inbox_p[g * bands : (g + 1) * bands].astype(F32)
        for c in range(2):
            right_f[c] = right[:, :, c * width : (c + 1) * width].reshape(bands * rows, width)
        result = jnp.zeros((bands, 4 * bands), F32)
        for r in range(rows):
            every = pl.ds(r, bands, stride=rows)
            low_re, low_im = left_f[0, every, :], left_f[1, every, :]
            high_re, high_im = right_f[0, every, :], right_f[1, every, :]
            low = jnp.concatenate([low_re, low_im], axis=1)
            stack = jnp.concatenate(
                [
                    jnp.concatenate([high_re, high_im], axis=1),
                    jnp.concatenate([high_im, -high_re], axis=1),
                    low,
                    jnp.concatenate([low_im, -low_re], axis=1),
                ],
                axis=0,
            )
            result += dot_nt(low.astype(BF16), stack.astype(BF16))
        result = result * (1.0 / float(4 * radius * radius))
        fold = message.shape[1] // (4 * bands)
        depth = message.shape[0]
        message[...] = jnp.concatenate(
            [result[f * depth : (f + 1) * depth] for f in range(fold)], axis=1
        )
        inbox_s[number] = message[...]
        b_each(lambda copy: copy.start())
        most = inbox_s.at[pl.ds(0, reducers - 1)]
        pltpu.make_async_copy(most, most, b_recv).wait()

    @pl.when(jnp.logical_not(is_reducer))
    def _():
        pltpu.make_async_copy(inbox_s, inbox_s, b_recv).wait()

    final = inbox_s[0]
    for r in range(1, reducers):
        final += inbox_s[r]
    span = 4 * bands
    fold = message.shape[1] // span
    final = jnp.concatenate([final[:, f * span : (f + 1) * span] for f in range(fold)], axis=0)
    red_ref[0] = final[:, :bands]
    red_ref[1] = final[:, bands : 2 * bands]
    corr_ref[0] = final[:, 2 * bands : 3 * bands]
    corr_ref[1] = final[:, 3 * bands :]

    m_each(lambda copy: copy.wait_send(), False)
    p_each(lambda copy: copy.wait_send(), False)

    @pl.when(is_reducer)
    def _():
        b_each(lambda copy: copy.wait_send())


def write_out(out_ref, corr_ref, red_ref, out_hbm, corr_hbm, red_hbm, sem):
    copies = [
        pltpu.make_async_copy(out_ref, out_hbm, sem.at[0]),
        pltpu.make_async_copy(corr_ref, corr_hbm, sem.at[1]),
        pltpu.make_async_copy(red_ref, red_hbm, sem.at[2]),
    ]
    for copy in copies:
        copy.start()
    for copy in copies:
        copy.wait()


def body(bands, groups, orbitals, potential, slot_sticks, stick_entries):
    points = potential.shape[1]
    planes = potential.shape[0]
    width = stick_entries.shape[1]
    radius = width // 2
    slots = orbitals.shape[2]
    plane_pad = -(-planes // 128) * 128
    coarse = 2 * width
    reducers = width // 16
    per_group = reducers // groups
    rows = width // reducers
    fold = max(1, 128 // (4 * bands))
    slot_lanes = -(-groups * slots // 128) * 128
    tz, tx, ty, tr = tables(points, width, radius, groups, planes, plane_pad, coarse)
    vmem = pl.BlockSpec(memory_space=pltpu.VMEM)
    hbm = pl.BlockSpec(memory_space=pltpu.HBM)
    total = bands * groups
    dma = pltpu.SemaphoreType.DMA
    results = pl.pallas_call(
        functools.partial(kernel, bands, groups, points, radius),
        out_shape=(
            pltpu.VMEM(orbitals.shape, BF16),
            pltpu.VMEM((2, bands, bands), F32),
            pltpu.VMEM((2, bands, bands), F32),
        ),
        in_specs=[hbm] * 8,
        out_specs=(vmem, vmem, vmem),
        scratch_shapes=[
            pltpu.VMEM(orbitals.shape, BF16),
            pltpu.VMEM(slot_sticks.shape, jnp.int32),
            pltpu.VMEM(stick_entries.shape, jnp.int32),
            pltpu.VMEM(tz.shape[1:], BF16),
            pltpu.VMEM(tx.shape, BF16),
            pltpu.VMEM(ty.shape, BF16),
            pltpu.VMEM(tr.shape, BF16),
            pltpu.VMEM((plane_pad, points), F32),
            pltpu.VMEM((width, slot_lanes), F32),
            pltpu.VMEM((groups, slots, width), jnp.int32),
            pltpu.VMEM((groups - 1, 2, slots, width), BF16),
            pltpu.VMEM((groups, slots, 2 * width), BF16),
            pltpu.VMEM((2, 2 * width, plane_pad), BF16),
            pltpu.VMEM((groups - 1, slots, 2 * width), F32),
            pltpu.VMEM((groups - 1, slots, 2 * width), F32),
            pltpu.VMEM((width, 2 * width), BF16),
            pltpu.VMEM((width, 2 * width), BF16),
            pltpu.VMEM((bands, rows, 2 * width), BF16),
            pltpu.VMEM((total, rows, 2 * width), BF16),
            pltpu.VMEM((2, bands * rows, width), F32),
            pltpu.VMEM((2, bands * rows, width), F32),
            pltpu.VMEM((bands // fold, 4 * bands * fold), F32),
            pltpu.VMEM((reducers, bands // fold, 4 * bands * fold), F32),
            dma((8,)),
            pltpu.SemaphoreType.REGULAR((2,)),
            dma((groups - 1,)),
            dma((groups - 1,)),
            dma((groups - 1,)),
            dma((groups - 1,)),
            dma((per_group,)),
            dma,
            dma((reducers,)),
            dma,
            dma((total,)),
            dma,
        ],
        compiler_params=pltpu.CompilerParams(
            collective_id=0, has_side_effects=True, vmem_limit_bytes=60000000
        ),
    )(orbitals, slot_sticks, stick_entries, potential, tz, tx, ty, tr)
    return pl.pallas_call(
        write_out,
        out_shape=[jax.ShapeDtypeStruct(r.shape, r.dtype) for r in results],
        in_specs=[vmem] * 3,
        out_specs=[hbm] * 3,
        scratch_shapes=[dma((3,))],
    )(*[pltpu.with_memory_space_constraint(r, pltpu.VMEM) for r in results])


def solution(mesh):
    bands = mesh.shape["band"]
    groups = mesh.shape["ga"]
    return jax.shard_map(
        functools.partial(body, bands, groups),
        mesh=mesh,
        in_specs=(P(None, "band", "ga", None), P("ga", None), P(), P()),
        out_specs=(P(None, "band", "ga", None), P(), P()),
        check_vma=False,
    )
```

```python
import functools
import math

import jax
import jax.numpy as jnp
import numpy as np
from jax import lax
from jax.experimental import pallas as pl
from jax.experimental.pallas import tpu as pltpu
from jax.sharding import PartitionSpec as P

MESH = pl.DeviceIdType.MESH
NT = (((1,), (1,)), ((), ()))
BF16 = jnp.bfloat16
F32 = jnp.float32
BLOCK = 4
UNROLL = 8


def split_np(table):
    high = table.astype(np.float32).astype(BF16)
    low = (table - high.astype(np.float64)).astype(np.float32).astype(BF16)
    return np.stack([high, low])


def triple(pair, axis):
    high, low = (np.take(pair, i, axis=pair.ndim - 3) for i in range(2))
    return np.concatenate([high, high, low], axis=axis)


def tables(points, width, radius, groups, planes, plane_pad, coarse):
    freq = np.arange(width) - radius + 1
    used = (np.arange(width) < width - 1).astype(np.float64)
    z_tabs = []
    for group in range(groups):
        z = np.arange(planes) + group * planes
        angle = 2.0 * np.pi * ((freq[:, None] * z[None, :]) % points) / points
        cos = np.zeros((width, plane_pad))
        sin = np.zeros((width, plane_pad))
        cos[:, :planes] = np.cos(angle) * used[:, None]
        sin[:, :planes] = np.sin(angle) * used[:, None]
        z_tabs.append(split_np(np.block([[cos, sin], [-sin, cos]])))
    x = np.arange(coarse)
    angle = 2.0 * np.pi * ((freq[None, :] * x[:, None]) % coarse) / coarse
    cos = np.cos(angle) * used[None, :]
    sin = np.sin(angle) * used[None, :]
    forward = np.block([[cos, -sin], [sin, cos]])
    limit = 2 * (radius - 1)
    offset = (x[:, None] * points - np.arange(points)[None, :] * coarse) % (coarse * points)
    base = 2.0 * np.pi * offset / (coarse * points)
    resample = np.ones((coarse, points))
    for g in range(1, limit + 1):
        resample += 2.0 * np.cos(g * base)
    resample /= points
    z_tabs = np.stack(z_tabs)
    return (
        z_tabs.reshape(groups, 2 * z_tabs.shape[2], z_tabs.shape[3]),
        triple(np.swapaxes(z_tabs, 2, 3), 1),
        triple(split_np(forward), 1),
        triple(split_np(forward.T.copy()), 1),
        split_np(resample),
    )


def split(value):
    high = value.astype(BF16)
    low = (value - high.astype(F32)).astype(BF16)
    return high, low


def thirds(value, axis):
    high, low = split(value)
    return jnp.concatenate([high, low, high], axis=axis)


def dot(a, b):
    return jnp.dot(a, b, preferred_element_type=F32)


def dot_nt(a, b):
    return lax.dot_general(a, b, NT, preferred_element_type=F32)


def take_lanes(value, index):
    return jnp.take_along_axis(value, index, axis=1, mode="promise_in_bounds")


def kernel(
    bands,
    groups,
    points,
    radius,
    orb_hbm,
    slots_hbm,
    entries_hbm,
    pot_hbm,
    tz_hbm,
    tb_hbm,
    tx_hbm,
    ty_hbm,
    tr_hbm,
    out_ref,
    corr_ref,
    red_ref,
    orb_ref,
    slots_ref,
    entries_ref,
    tz,
    tb,
    tx,
    ty,
    tr,
    pot,
    ent_t,
    inv_ref,
    raw,
    spread,
    part,
    got,
    dense_ref,
    pdense,
    inbox_m,
    inbox_p,
    left_f,
    right_f,
    message,
    inbox_s,
    load_sem,
    near_sem,
    pair_sem,
    s_send,
    s_recv,
    x_send,
    x_recv,
    m_send,
    m_recv,
    p_send,
    p_recv,
    b_send,
    b_recv,
):
    band = lax.axis_index("band")
    ga = lax.axis_index("ga")
    total = bands * groups
    me = ga * bands + band
    slots = orb_hbm.shape[2]
    width = orb_hbm.shape[3]
    planes = pot_hbm.shape[0]
    plane_pad = pot.shape[0]
    coarse = tx.shape[0] // 2
    reducers = inbox_s.shape[0]
    rows = width // reducers
    per_group = reducers // groups
    block = math.gcd(bands, BLOCK)
    blocks = bands // block
    place = lax.rem(band, block)
    base = band - place
    first_band = bands // 2 - per_group + 1

    loads = [
        pltpu.make_async_copy(entries_hbm, entries_ref, load_sem.at[5]),
        pltpu.make_async_copy(orb_hbm, orb_ref, load_sem.at[6]),
        pltpu.make_async_copy(slots_hbm, slots_ref, load_sem.at[7]),
        pltpu.make_async_copy(pot_hbm, pot.at[pl.ds(0, planes)], load_sem.at[0]),
        pltpu.make_async_copy(tr_hbm, tr, load_sem.at[1]),
        pltpu.make_async_copy(tz_hbm.at[ga], tz, load_sem.at[2]),
        pltpu.make_async_copy(tx_hbm, tx, load_sem.at[3]),
        pltpu.make_async_copy(ty_hbm, ty, load_sem.at[4]),
        pltpu.make_async_copy(tb_hbm.at[ga], tb, load_sem.at[8]),
    ]
    load_entries, load_orb, load_slots, load_pot, load_tr, load_tz, load_tx, load_ty, load_tb = loads
    load_orb.start()

    has_low = band >= block
    has_high = band < bands - block
    barrier = pltpu.get_barrier_semaphore()
    for c in range(block):
        for g in range(groups):
            if g or c:
                pl.semaphore_signal(
                    barrier,
                    inc=1,
                    device_id=(base + lax.rem(place + c, block), lax.rem(ga + g, groups)),
                    device_id_type=MESH,
                )

    def near(semaphore_low, semaphore_high):
        @pl.when(has_low)
        def _():
            pl.semaphore_signal(
                semaphore_high, inc=1, device_id=(band - block, ga), device_id_type=MESH
            )

        @pl.when(has_high)
        def _():
            pl.semaphore_signal(
                semaphore_low, inc=1, device_id=(band + block, ga), device_id_type=MESH
            )

    def near_wait():
        @pl.when(has_low)
        def _():
            pl.semaphore_wait(near_sem.at[0], 1)

        @pl.when(has_high)
        def _():
            pl.semaphore_wait(near_sem.at[1], 1)

    near(barrier, barrier)
    for load in loads:
        if load is not load_orb:
            load.start()
    if plane_pad > planes:
        pot[pl.ds(planes, plane_pad - planes), :] = jnp.zeros(
            (plane_pad - planes, pot.shape[1]), F32
        )

    load_orb.wait()
    pl.semaphore_wait(
        barrier, block * groups - 1 + has_low.astype(jnp.int32) + has_high.astype(jnp.int32)
    )
    s_copies = []
    for k in range(1, groups):
        copy = pltpu.make_async_remote_copy(
            src_ref=orb_ref.at[:, 0],
            dst_ref=raw.at[k - 1],
            send_sem=s_send.at[k - 1],
            recv_sem=s_recv.at[k - 1],
            device_id=(band, lax.rem(ga + k, groups)),
            device_id_type=MESH,
        )
        copy.start()
        s_copies.append(copy)
    near(near_sem.at[0], near_sem.at[1])

    load_entries.wait()
    load_slots.wait()
    all_slots = groups * slots
    listed = entries_ref[...].astype(F32)
    slot_pad = ent_t.shape[1] - all_slots
    if slot_pad:
        listed = jnp.concatenate([listed, jnp.full((slot_pad, width), -1.0, F32)], axis=0)
    ent_t[...] = listed.T
    lanes = ent_t.shape[1]
    which = lax.broadcasted_iota(jnp.int32, (width, lanes), 0).astype(F32).astype(BF16)

    def invert(step, found):
        for u in range(UNROLL):
            k = step * UNROLL + u
            row = jnp.broadcast_to(ent_t[pl.ds(k, 1), :], (16, lanes)).astype(BF16)
            row = jnp.concatenate([row] * (width // 16), axis=0)
            found = jnp.where(row == which, k.astype(F32).astype(BF16), found)
        return found

    found = lax.fori_loop(
        0, width // UNROLL, invert, jnp.full((width, lanes), -1.0, BF16)
    )
    found = found.astype(F32).T.astype(jnp.int32)
    for g in range(groups):
        inv_ref[g] = found[g * slots : (g + 1) * slots]

    def spread_of(g, re, im):
        inverse = inv_ref[g]
        filled = inverse >= 0
        index = jnp.maximum(inverse, 0)
        spread[g, :, :width] = jnp.where(filled, take_lanes(re, index), 0.0).astype(BF16)
        spread[g, :, width:] = jnp.where(filled, take_lanes(im, index), 0.0).astype(BF16)

    re = orb_ref[0, 0].astype(F32)
    im = orb_ref[1, 0].astype(F32)
    spread_of(ga, re, im)

    near_wait()
    rounds = max(blocks // 2, 1)
    if rounds > 1:
        near(near_sem.at[0], near_sem.at[1])

    load_pot.wait()
    load_tr.wait()
    pot_hi, pot_lo = split(pot[...])
    weight = dot_nt(tr[0], pot_hi) + dot_nt(tr[0], pot_lo) + dot_nt(tr[1], pot_hi)

    for k, copy in enumerate(s_copies, 1):
        copy.wait()
        spread_of(
            lax.rem(ga - k + groups, groups), raw[k - 1, 0].astype(F32), raw[k - 1, 1].astype(F32)
        )
    all_sticks = slots_ref[...].reshape(1, all_slots)
    sticks = [all_sticks[:, g * slots : (g + 1) * slots] for g in range(groups)]
    dense = jnp.zeros((width, 2 * width), F32)
    sub = lax.broadcasted_iota(jnp.int32, (width, slots), 0)
    for g in range(groups):
        choose = jnp.where(sub == sticks[g], 1.0, 0.0).astype(BF16)
        dense += dot(choose, spread[g])
    dense = dense.astype(BF16)
    dense_ref[...] = dense

    for r in range(1, rounds):
        near_wait()
        if r < rounds - 1:
            near(near_sem.at[0], near_sem.at[1])

    def place_of(r):
        return first_band + 2 * lax.rem(r, per_group), lax.div(r, per_group)

    def m_copy(q):
        start = pl.multiple_of((ga * per_group + q) * rows, rows)
        return pltpu.make_async_remote_copy(
            src_ref=dense_ref.at[pl.ds(start, rows)],
            dst_ref=inbox_m.at[band],
            send_sem=m_send.at[q],
            recv_sem=m_recv,
            device_id=(first_band + 2 * q, ga),
            device_id_type=MESH,
        )

    def m_each(act, own):
        for q in range(per_group):
            mine = band == first_band + 2 * q

            @pl.when(jnp.logical_not(mine))
            def _(q=q):
                act(m_copy(q))

            if own:

                @pl.when(mine)
                def _(q=q):
                    start = pl.multiple_of((ga * per_group + q) * rows, rows)
                    inbox_m[band] = dense_ref[pl.ds(start, rows), :]

    m_each(lambda copy: copy.start(), True)

    load_tz.wait()
    pair = jnp.concatenate([dense, dense], axis=1)
    columns = [dot(pair, tz[:, :plane_pad]), dot(pair, tz[:, plane_pad:])]
    columns = jnp.concatenate(columns, axis=0)
    load_tx.wait()
    columns = thirds(columns, 0)
    quarter = coarse // 2
    field = jnp.concatenate(
        [dot(tx[i * quarter : (i + 1) * quarter], columns) for i in range(4)], axis=0
    )
    product = jnp.concatenate([field[:coarse] * weight, field[coarse:] * weight], axis=0)
    product = thirds(product, 0)
    load_ty.wait()
    back = jnp.concatenate([dot(ty[:width], product), dot(ty[width:], product)], axis=0)
    back = thirds(jnp.concatenate([back[:width], back[width:]], axis=1), 1)
    load_tb.wait()
    spectra = dot(back, tb[...])
    spectra = spectra * (1.0 / float(points * coarse))
    spec_hi, spec_lo = split(spectra)
    pdense[...] = spec_hi

    nearest = jnp.where(
        band >= bands // 2, per_group // 2 + lax.div(lax.rem(band, block), 2), lax.div(lax.rem(band, block), 2)
    )
    nearest = lax.rem(nearest, per_group)

    def far_reducer(far):
        g = lax.rem(ga + far // per_group, groups)
        q, bit = 0, 1
        while bit < per_group:
            own_bit = lax.rem(lax.div(nearest, bit), 2)
            q = q + bit * (1 - own_bit if far % per_group & bit else own_bit)
            bit *= 2
        return g * per_group + q

    def p_copy(r):
        return pltpu.make_async_remote_copy(
            src_ref=pdense.at[pl.ds(pl.multiple_of(r * rows, rows), rows)],
            dst_ref=inbox_p.at[me],
            send_sem=p_send.at[r],
            recv_sem=p_recv,
            device_id=place_of(r),
            device_id_type=MESH,
        )

    def p_each(act, own):
        for far in reversed(range(reducers)):
            r = far_reducer(far)
            to_band, to_ga = place_of(r)
            mine = me == to_ga * bands + to_band

            @pl.when(jnp.logical_not(mine))
            def _(r=r):
                act(p_copy(r))

            if own:

                @pl.when(mine)
                def _(r=r):
                    inbox_p[me] = pdense[pl.ds(pl.multiple_of(r * rows, rows), rows), :]

    p_each(lambda copy: copy.start(), True)

    @pl.when(lax.rem(band, 2) == 0)
    def _():
        pl.semaphore_signal(pair_sem, inc=1, device_id=(band + 1, ga), device_id_type=MESH)

    eye = lax.broadcasted_iota(jnp.int32, (slots, slots), 0) == lax.broadcasted_iota(
        jnp.int32, (slots, slots), 1
    )

    def stick_column(g):
        row = sticks[0]
        for other in range(1, groups):
            row = jnp.where(g == other, sticks[other], row)
        row = row.astype(F32)
        return jnp.sum(jnp.where(eye, row, 0.0), axis=1, keepdims=True)

    lane = lax.broadcasted_iota(jnp.int32, (slots, width), 1)
    lane_f = lane.astype(F32)
    x_copies = []
    for k in range(1, groups + 1):
        target = lax.rem(ga + k, groups)
        stick = stick_column(target)
        choose = jnp.where(stick == lane_f, 1.0, 0.0).astype(BF16)
        mine = dot(choose, spec_hi) + dot(choose, spec_lo)
        if k < groups:
            part[k - 1] = mine
            copy = pltpu.make_async_remote_copy(
                src_ref=part.at[k - 1],
                dst_ref=got.at[k - 1],
                send_sem=x_send.at[k - 1],
                recv_sem=x_recv.at[k - 1],
                device_id=(band, target),
                device_id_type=MESH,
            )
            x_copies.append(copy)

    own = entries_ref[pl.ds(pl.multiple_of(ga * slots, 8), slots)]
    present = own >= 0
    gx = stick - float(radius - 1)
    gz = (own - (radius - 1)).astype(F32)
    kinetic = (gx * gx + gz * gz) * (1.0 / float(radius * radius))
    own_index = jnp.maximum(own, 0)

    @pl.when(lax.rem(band, 2) == 1)
    def _():
        pl.semaphore_wait(pair_sem, 1)

    for copy in x_copies:
        copy.start()

    offset = band - first_band
    is_reducer = (offset >= 0) & (offset < 2 * per_group) & (lax.rem(band + 1, 2) == 0)
    number = ga * per_group + lax.div(jnp.clip(offset, 0, 2 * per_group - 1), 2)

    def b_copy(t):
        return pltpu.make_async_remote_copy(
            src_ref=message,
            dst_ref=inbox_s.at[number],
            send_sem=b_send.at[t],
            recv_sem=b_recv,
            device_id=(t // groups, t % groups) if isinstance(t, int) else (lax.div(t, groups), lax.rem(t, groups)),
            device_id_type=MESH,
        )

    def b_each(act):
        order = band * groups + ga
        if total <= 64:
            for t in range(total):

                @pl.when(order != t)
                def _(t=t):
                    act(b_copy(t))
        else:

            @pl.loop(0, total)
            def _(t):
                @pl.when(order != t)
                def _():
                    act(b_copy(t))

    def keep(ref, value):
        for c in range(2):
            ref[c] = value[:, :, c * width : (c + 1) * width].reshape(bands * rows, width)

    @pl.when(is_reducer)
    def _():
        m_all = inbox_m.at[pl.ds(0, bands - 1)]
        pltpu.make_async_copy(m_all, m_all, m_recv).wait()
        left = inbox_m[...].astype(F32)
        row_id = lax.broadcasted_iota(jnp.int32, (rows, 2 * width), 0) + number * rows
        lane_id = lax.broadcasted_iota(jnp.int32, (rows, 2 * width), 1)
        row_f = (row_id - (radius - 1)).astype(F32)
        lane_g = (jnp.where(lane_id >= width, lane_id - width, lane_id) - (radius - 1)).astype(F32)
        kin = (row_f * row_f + lane_g * lane_g) * (1.0 / float(radius * radius))
        right = left * kin[None]
        keep(left_f, left)

        def overlaps(source):
            result = jnp.zeros((2 * bands, bands), F32)
            for r in range(rows):
                every = pl.ds(r, bands, stride=rows)
                low = jnp.concatenate([left_f[0, every, :], left_f[1, every, :]], axis=1)
                high_re, high_im = source[0, every, :], source[1, every, :]
                stack = jnp.concatenate(
                    [
                        jnp.concatenate([high_re, high_im], axis=1),
                        jnp.concatenate([-high_im, high_re], axis=1),
                    ],
                    axis=0,
                )
                result += dot_nt(stack.astype(BF16), low.astype(BF16))
            return result * (1.0 / float(4 * radius * radius))

        corr = overlaps(left_f)
        p_all = inbox_p.at[pl.ds(0, total - 1)]
        pltpu.make_async_copy(p_all, p_all, p_recv).wait()
        for g in range(groups):
            right += inbox_p[g * bands : (g + 1) * bands].astype(F32)
        keep(right_f, right)
        result = jnp.concatenate([overlaps(right_f), corr], axis=0)
        depth = message.shape[0]
        message[...] = jnp.concatenate(
            [result[f : f + depth] for f in range(0, 4 * bands, depth)], axis=1
        )
        inbox_s[number] = message[...]
        b_each(lambda copy: copy.start())

    for copy in x_copies:
        copy.wait()
    for k in range(1, groups):
        mine += got[k - 1]
    a_re = take_lanes(mine[:, :width], own_index)
    a_im = take_lanes(mine[:, width:], own_index)
    out_ref[0, 0] = jnp.where(present, kinetic * re + a_re, 0.0).astype(BF16)
    out_ref[1, 0] = jnp.where(present, kinetic * im + a_im, 0.0).astype(BF16)

    m_each(lambda copy: copy.wait_send(), False)
    p_each(lambda copy: copy.wait_send(), False)

    @pl.when(is_reducer)
    def _():
        most = inbox_s.at[pl.ds(0, reducers - 1)]
        pltpu.make_async_copy(most, most, b_recv).wait()

    @pl.when(jnp.logical_not(is_reducer))
    def _():
        pltpu.make_async_copy(inbox_s, inbox_s, b_recv).wait()

    final = inbox_s[0]
    for r in range(1, reducers):
        final += inbox_s[r]
    final = jnp.concatenate(
        [final[:, f : f + bands] for f in range(0, final.shape[1], bands)], axis=0
    )
    red_ref[0] = final[:bands]
    red_ref[1] = final[bands : 2 * bands]
    corr_ref[0] = final[2 * bands : 3 * bands]
    corr_ref[1] = final[3 * bands :]


    @pl.when(is_reducer)
    def _():
        b_each(lambda copy: copy.wait_send())


def write_out(out_ref, corr_ref, red_ref, out_hbm, corr_hbm, red_hbm, sem):
    copies = [
        pltpu.make_async_copy(out_ref, out_hbm, sem.at[0]),
        pltpu.make_async_copy(corr_ref, corr_hbm, sem.at[1]),
        pltpu.make_async_copy(red_ref, red_hbm, sem.at[2]),
    ]
    for copy in copies:
        copy.start()
    for copy in copies:
        copy.wait()


def body(bands, groups, orbitals, potential, slot_sticks, stick_entries):
    points = potential.shape[1]
    planes = potential.shape[0]
    width = stick_entries.shape[1]
    radius = width // 2
    slots = orbitals.shape[2]
    plane_pad = -(-planes // 128) * 128
    coarse = 2 * width
    reducers = width // 16
    per_group = reducers // groups
    rows = width // reducers
    fold = max(1, 128 // bands)
    slot_lanes = -(-groups * slots // 128) * 128
    tz, tb, tx, ty, tr = tables(points, width, radius, groups, planes, plane_pad, coarse)
    vmem = pl.BlockSpec(memory_space=pltpu.VMEM)
    hbm = pl.BlockSpec(memory_space=pltpu.HBM)
    total = bands * groups
    dma = pltpu.SemaphoreType.DMA
    results = pl.pallas_call(
        functools.partial(kernel, bands, groups, points, radius),
        out_shape=(
            pltpu.VMEM(orbitals.shape, BF16),
            pltpu.VMEM((2, bands, bands), F32),
            pltpu.VMEM((2, bands, bands), F32),
        ),
        in_specs=[hbm] * 9,
        out_specs=(vmem, vmem, vmem),
        scratch_shapes=[
            pltpu.VMEM(orbitals.shape, BF16),
            pltpu.VMEM(slot_sticks.shape, jnp.int32),
            pltpu.VMEM(stick_entries.shape, jnp.int32),
            pltpu.VMEM(tz.shape[1:], BF16),
            pltpu.VMEM(tb.shape[1:], BF16),
            pltpu.VMEM(tx.shape, BF16),
            pltpu.VMEM(ty.shape, BF16),
            pltpu.VMEM(tr.shape, BF16),
            pltpu.VMEM((plane_pad, points), F32),
            pltpu.VMEM((width, slot_lanes), F32),
            pltpu.VMEM((groups, slots, width), jnp.int32),
            pltpu.VMEM((groups - 1, 2, slots, width), BF16),
            pltpu.VMEM((groups, slots, 2 * width), BF16),
            pltpu.VMEM((groups - 1, slots, 2 * width), F32),
            pltpu.VMEM((groups - 1, slots, 2 * width), F32),
            pltpu.VMEM((width, 2 * width), BF16),
            pltpu.VMEM((width, 2 * width), BF16),
            pltpu.VMEM((bands, rows, 2 * width), BF16),
            pltpu.VMEM((total, rows, 2 * width), BF16),
            pltpu.VMEM((2, bands * rows, width), F32),
            pltpu.VMEM((2, bands * rows, width), F32),
            pltpu.VMEM((4 * bands // fold, bands * fold), F32),
            pltpu.VMEM((reducers, 4 * bands // fold, bands * fold), F32),
            dma((9,)),
            pltpu.SemaphoreType.REGULAR((2,)),
            pltpu.SemaphoreType.REGULAR,
            dma((groups - 1,)),
            dma((groups - 1,)),
            dma((groups - 1,)),
            dma((groups - 1,)),
            dma((per_group,)),
            dma,
            dma((reducers,)),
            dma,
            dma((total,)),
            dma,
        ],
        compiler_params=pltpu.CompilerParams(
            collective_id=0, has_side_effects=True, vmem_limit_bytes=60000000
        ),
    )(orbitals, slot_sticks, stick_entries, potential, tz, tb, tx, ty, tr)
    return pl.pallas_call(
        write_out,
        out_shape=[jax.ShapeDtypeStruct(r.shape, r.dtype) for r in results],
        in_specs=[vmem] * 3,
        out_specs=[hbm] * 3,
        scratch_shapes=[dma((3,))],
    )(*[pltpu.with_memory_space_constraint(r, pltpu.VMEM) for r in results])


def solution(mesh):
    bands = mesh.shape["band"]
    groups = mesh.shape["ga"]
    return jax.shard_map(
        functools.partial(body, bands, groups),
        mesh=mesh,
        in_specs=(P(None, "band", "ga", None), P("ga", None), P(), P()),
        out_specs=(P(None, "band", "ga", None), P(), P()),
        check_vma=False,
    )
```

```python
import functools
import math

import jax
import jax.numpy as jnp
import numpy as np
from jax import lax
from jax.experimental import pallas as pl
from jax.experimental.pallas import tpu as pltpu
from jax.sharding import PartitionSpec as P

MESH = pl.DeviceIdType.MESH
NT = (((1,), (1,)), ((), ()))
BF16 = jnp.bfloat16
F32 = jnp.float32
BLOCK = 4
UNROLL = 8


def split_np(table):
    high = table.astype(np.float32).astype(BF16)
    low = (table - high.astype(np.float64)).astype(np.float32).astype(BF16)
    return np.stack([high, low])


def tables(points, width, radius, groups, planes, plane_pad, coarse):
    freq = np.arange(width) - radius + 1
    used = (np.arange(width) < width - 1).astype(np.float64)
    z_tabs = []
    for group in range(groups):
        z = np.arange(planes) + group * planes
        angle = 2.0 * np.pi * ((freq[:, None] * z[None, :]) % points) / points
        cos = np.zeros((width, plane_pad))
        sin = np.zeros((width, plane_pad))
        cos[:, :planes] = np.cos(angle) * used[:, None]
        sin[:, :planes] = np.sin(angle) * used[:, None]
        z_tabs.append(split_np(np.block([[cos, sin], [-sin, cos]])))
    x = np.arange(coarse)
    angle = 2.0 * np.pi * ((freq[None, :] * x[:, None]) % coarse) / coarse
    cos = np.cos(angle) * used[None, :]
    sin = np.sin(angle) * used[None, :]
    forward = np.block([[cos, -sin], [sin, cos]])
    limit = 2 * (radius - 1)
    offset = (x[:, None] * points - np.arange(points)[None, :] * coarse) % (coarse * points)
    base = 2.0 * np.pi * offset / (coarse * points)
    resample = np.ones((coarse, points))
    for g in range(1, limit + 1):
        resample += 2.0 * np.cos(g * base)
    resample /= points
    z_tabs = np.stack(z_tabs)
    return (
        z_tabs,
        np.swapaxes(z_tabs, 2, 3).copy(),
        split_np(forward),
        split_np(forward.T.copy()),
        split_np(resample),
    )


def split(value):
    high = value.astype(BF16)
    low = (value - high.astype(F32)).astype(BF16)
    return high, low


def thirds(value, axis):
    high, low = split(value)
    return jnp.concatenate([high, low, high], axis=axis)


def dot(a, b):
    return jnp.dot(a, b, preferred_element_type=F32)


def dot_nt(a, b):
    return lax.dot_general(a, b, NT, preferred_element_type=F32)


def take_lanes(value, index):
    return jnp.take_along_axis(value, index, axis=1, mode="promise_in_bounds")


def kernel(
    bands,
    groups,
    points,
    radius,
    orb_hbm,
    slots_hbm,
    entries_hbm,
    pot_hbm,
    tz_hbm,
    tb_hbm,
    tx_hbm,
    ty_hbm,
    tr_hbm,
    out_ref,
    corr_ref,
    red_ref,
    orb_ref,
    slots_ref,
    entries_ref,
    tz,
    tb,
    tx,
    ty,
    tr,
    pot,
    ent_t,
    inv_ref,
    raw,
    spread,
    part,
    got,
    dense_ref,
    pdense,
    inbox_m,
    inbox_p,
    left_f,
    right_f,
    message,
    inbox_s,
    load_sem,
    near_sem,
    pair_sem,
    s_send,
    s_recv,
    x_send,
    x_recv,
    m_send,
    m_recv,
    p_send,
    p_recv,
    b_send,
    b_recv,
):
    band = lax.axis_index("band")
    ga = lax.axis_index("ga")
    total = bands * groups
    twin = band + 1 - 2 * lax.rem(band, 2)
    me = ga * bands + twin
    slots = orb_hbm.shape[2]
    width = orb_hbm.shape[3]
    planes = pot_hbm.shape[0]
    plane_pad = pot.shape[0]
    coarse = tx.shape[1] // 2
    reducers = inbox_s.shape[0]
    rows = width // reducers
    per_group = reducers // groups
    block = math.gcd(bands, BLOCK)
    blocks = bands // block
    place = lax.rem(band, block)
    base = band - place
    first_band = bands // 2 - per_group + 1

    loads = [
        pltpu.make_async_copy(entries_hbm, entries_ref, load_sem.at[5]),
        pltpu.make_async_copy(orb_hbm, orb_ref, load_sem.at[6]),
        pltpu.make_async_copy(slots_hbm, slots_ref, load_sem.at[7]),
        pltpu.make_async_copy(pot_hbm, pot.at[pl.ds(0, planes)], load_sem.at[0]),
        pltpu.make_async_copy(tr_hbm, tr, load_sem.at[1]),
        pltpu.make_async_copy(tz_hbm.at[ga], tz, load_sem.at[2]),
        pltpu.make_async_copy(tx_hbm, tx, load_sem.at[3]),
        pltpu.make_async_copy(ty_hbm, ty, load_sem.at[4]),
        pltpu.make_async_copy(tb_hbm.at[ga], tb, load_sem.at[8]),
    ]
    load_entries, load_orb, load_slots, load_pot, load_tr, load_tz, load_tx, load_ty, load_tb = loads
    load_orb.start()

    has_low = band >= block
    has_high = band < bands - block
    barrier = pltpu.get_barrier_semaphore()
    across = band + 2 - 4 * lax.rem(lax.div(band, 2), 2)

    def greet(to_band, to_ga, semaphore=barrier):
        pl.semaphore_signal(semaphore, inc=1, device_id=(to_band, to_ga), device_id_type=MESH)

    for k in range(1, groups):
        greet(twin, lax.rem(ga + k, groups))
        greet(band, lax.rem(ga + k, groups))
    greet(twin, ga)
    greet(across, ga)

    def near(semaphore_low, semaphore_high):
        @pl.when(has_low)
        def _():
            pl.semaphore_signal(
                semaphore_high, inc=1, device_id=(band - block, ga), device_id_type=MESH
            )

        @pl.when(has_high)
        def _():
            pl.semaphore_signal(
                semaphore_low, inc=1, device_id=(band + block, ga), device_id_type=MESH
            )

    def near_wait():
        @pl.when(has_low)
        def _():
            pl.semaphore_wait(near_sem.at[0], 1)

        @pl.when(has_high)
        def _():
            pl.semaphore_wait(near_sem.at[1], 1)

    near(barrier, barrier)
    for load in loads:
        if load is not load_orb:
            load.start()
    if plane_pad > planes:
        pot[pl.ds(planes, plane_pad - planes), :] = jnp.zeros(
            (plane_pad - planes, pot.shape[1]), F32
        )

    load_orb.wait()
    pl.semaphore_wait(
        barrier, 2 * groups + has_low.astype(jnp.int32) + has_high.astype(jnp.int32)
    )
    s_copies = []
    for k in range(1, groups + 1):
        copy = pltpu.make_async_remote_copy(
            src_ref=orb_ref.at[:, 0],
            dst_ref=raw.at[ga],
            send_sem=s_send.at[k - 1],
            recv_sem=s_recv.at[ga],
            device_id=(twin, lax.rem(ga + k, groups)),
            device_id_type=MESH,
        )
        copy.start()
        s_copies.append(copy)

    def arrived(ref, sem, g):
        pltpu.make_async_copy(ref.at[g], ref.at[g], sem.at[g]).wait()

    greet(across, ga, near_sem.at[2])

    load_entries.wait()
    load_slots.wait()
    all_slots = groups * slots
    listed = entries_ref[...].astype(F32)
    slot_pad = ent_t.shape[1] - all_slots
    if slot_pad:
        listed = jnp.concatenate([listed, jnp.full((slot_pad, width), -1.0, F32)], axis=0)
    ent_t[...] = listed.T
    lanes = ent_t.shape[1]
    which = lax.broadcasted_iota(jnp.int32, (width, lanes), 0).astype(F32).astype(BF16)

    def invert(step, found):
        for u in range(UNROLL):
            k = step * UNROLL + u
            row = jnp.broadcast_to(ent_t[pl.ds(k, 1), :], (16, lanes)).astype(BF16)
            row = jnp.concatenate([row] * (width // 16), axis=0)
            found = jnp.where(row == which, k.astype(F32).astype(BF16), found)
        return found

    found = lax.fori_loop(
        0, width // UNROLL, invert, jnp.full((width, lanes), -1.0, BF16)
    )
    found = found.astype(F32).T.astype(jnp.int32)
    for g in range(groups):
        inv_ref[g] = found[g * slots : (g + 1) * slots]

    def spread_of(g):
        arrived(raw, s_recv, g)
        re = raw[g, 0].astype(F32)
        im = raw[g, 1].astype(F32)
        inverse = inv_ref[g]
        filled = inverse >= 0
        index = jnp.maximum(inverse, 0)
        spread[g, :, :width] = jnp.where(filled, take_lanes(re, index), 0.0).astype(BF16)
        spread[g, :, width:] = jnp.where(filled, take_lanes(im, index), 0.0).astype(BF16)

    re = orb_ref[0, 0].astype(F32)
    im = orb_ref[1, 0].astype(F32)
    spread_of(ga)

    rounds = max(blocks // 2, 1)
    pl.semaphore_wait(near_sem.at[2], 1)
    near(near_sem.at[0], near_sem.at[1])

    load_pot.wait()
    load_tr.wait()
    pot_hi, pot_lo = split(pot[...])
    weight = dot_nt(tr[0], pot_hi) + dot_nt(tr[0], pot_lo) + dot_nt(tr[1], pot_hi)

    near_wait()
    if rounds > 1:
        near(near_sem.at[0], near_sem.at[1])

    for k in range(1, groups):
        spread_of(lax.rem(ga + k, groups))
    for copy in s_copies:
        copy.wait_send()
    all_sticks = slots_ref[...].reshape(1, all_slots)
    sticks = [all_sticks[:, g * slots : (g + 1) * slots] for g in range(groups)]
    dense = jnp.zeros((width, 2 * width), F32)
    sub = lax.broadcasted_iota(jnp.int32, (width, slots), 0)
    for g in range(groups):
        choose = jnp.where(sub == sticks[g], 1.0, 0.0).astype(BF16)
        dense += dot(choose, spread[g])
    dense = dense.astype(BF16)
    dense_ref[...] = dense

    for r in range(1, rounds):
        near_wait()
        if r < rounds - 1:
            near(near_sem.at[0], near_sem.at[1])

    def place_of(r):
        return first_band + 2 * lax.rem(r, per_group), lax.div(r, per_group)

    def other(to_band, to_ga):
        own = (to_band == band) & (to_ga == ga)
        return jnp.where(own, band - 1, to_band), to_ga

    m_copies = []
    for q in range(per_group):
        start = pl.multiple_of((ga * per_group + q) * rows, rows)
        m_copies.append(
            pltpu.make_async_remote_copy(
                src_ref=dense_ref.at[pl.ds(start, rows)],
                dst_ref=inbox_m.at[twin],
                send_sem=m_send.at[q],
                recv_sem=m_recv,
                device_id=other(first_band + 2 * q, ga),
                device_id_type=MESH,
            )
        )
        m_copies[-1].start()

    load_tz.wait()
    pair = jnp.concatenate([dense, dense], axis=1)
    z_table = jnp.concatenate([tz[0], tz[1]], axis=0)
    columns = [dot(pair, z_table[:, :plane_pad]), dot(pair, z_table[:, plane_pad:])]
    columns = jnp.concatenate(columns, axis=0)
    load_tx.wait()
    x_table = jnp.concatenate([tx[0], tx[0], tx[1]], axis=1)
    columns = thirds(columns, 0)
    quarter = coarse // 2
    field = jnp.concatenate(
        [dot(x_table[i * quarter : (i + 1) * quarter], columns) for i in range(4)], axis=0
    )
    product = jnp.concatenate([field[:coarse] * weight, field[coarse:] * weight], axis=0)
    product = thirds(product, 0)
    load_ty.wait()
    y_table = jnp.concatenate([ty[0], ty[0], ty[1]], axis=1)
    back = jnp.concatenate([dot(y_table[:width], product), dot(y_table[width:], product)], axis=0)
    back = thirds(jnp.concatenate([back[:width], back[width:]], axis=1), 1)
    load_tb.wait()
    spectra = dot(back, jnp.concatenate([tb[0], tb[0], tb[1]], axis=0))
    spectra = spectra * (1.0 / float(points * coarse))
    spec_hi, spec_lo = split(spectra)
    pdense[...] = spec_hi

    nearest = jnp.where(
        band >= bands // 2, per_group // 2 + lax.div(lax.rem(band, block), 2), lax.div(lax.rem(band, block), 2)
    )
    nearest = lax.rem(nearest, per_group)

    def far_reducer(far):
        g = lax.rem(ga + far // per_group, groups)
        q, bit = 0, 1
        while bit < per_group:
            own_bit = lax.rem(lax.div(nearest, bit), 2)
            q = q + bit * (1 - own_bit if far % per_group & bit else own_bit)
            bit *= 2
        return g * per_group + q

    p_copies = []
    for far in reversed(range(reducers)):
        r = far_reducer(far)
        p_copies.append(
            pltpu.make_async_remote_copy(
                src_ref=pdense.at[pl.ds(pl.multiple_of(r * rows, rows), rows)],
                dst_ref=inbox_p.at[me],
                send_sem=p_send.at[far],
                recv_sem=p_recv,
                device_id=other(*place_of(r)),
                device_id_type=MESH,
            )
        )
        p_copies[-1].start()

    @pl.when(lax.rem(band, 2) == 0)
    def _():
        pl.semaphore_signal(pair_sem, inc=1, device_id=(band + 1, ga), device_id_type=MESH)

    eye = lax.broadcasted_iota(jnp.int32, (slots, slots), 0) == lax.broadcasted_iota(
        jnp.int32, (slots, slots), 1
    )

    def stick_column(g):
        row = sticks[0]
        for other in range(1, groups):
            row = jnp.where(g == other, sticks[other], row)
        row = row.astype(F32)
        return jnp.sum(jnp.where(eye, row, 0.0), axis=1, keepdims=True)

    lane = lax.broadcasted_iota(jnp.int32, (slots, width), 1)
    lane_f = lane.astype(F32)
    x_copies = []
    for k in range(1, groups + 1):
        target = lax.rem(ga + k, groups)
        stick = stick_column(target)
        choose = jnp.where(stick == lane_f, 1.0, 0.0).astype(BF16)
        mine = dot(choose, spec_hi) + dot(choose, spec_lo)
        part[k - 1] = mine
        x_copies.append(
            pltpu.make_async_remote_copy(
                src_ref=part.at[k - 1],
                dst_ref=got.at[ga],
                send_sem=x_send.at[k - 1],
                recv_sem=x_recv.at[ga],
                device_id=(twin, target),
                device_id_type=MESH,
            )
        )

    own = entries_ref[pl.ds(pl.multiple_of(ga * slots, 8), slots)]
    present = own >= 0
    gx = stick - float(radius - 1)
    gz = (own - (radius - 1)).astype(F32)
    kinetic = (gx * gx + gz * gz) * (1.0 / float(radius * radius))
    own_index = jnp.maximum(own, 0)

    @pl.when(lax.rem(band, 2) == 1)
    def _():
        pl.semaphore_wait(pair_sem, 1)

    for copy in x_copies:
        copy.start()

    offset = band - first_band
    is_reducer = (offset >= 0) & (offset < 2 * per_group) & (lax.rem(band + 1, 2) == 0)
    number = ga * per_group + lax.div(jnp.clip(offset, 0, 2 * per_group - 1), 2)

    order = band * groups + ga

    def b_copy(t):
        if isinstance(t, int):
            to_band, to_ga = t // groups, t % groups
        else:
            to_band, to_ga = lax.div(t, groups), lax.rem(t, groups)
        return pltpu.make_async_remote_copy(
            src_ref=message,
            dst_ref=inbox_s.at[number],
            send_sem=b_send.at[t],
            recv_sem=b_recv,
            device_id=(to_band, to_ga),
            device_id_type=MESH,
        )

    def b_each(act):
        if total <= 64:
            for t in range(total):

                @pl.when(order != t)
                def _(t=t):
                    act(b_copy(t))
        else:

            @pl.loop(0, total)
            def _(t):
                @pl.when(order != t)
                def _():
                    act(b_copy(t))

    def keep(ref, value):
        for c in range(2):
            ref[c] = value[:, :, c * width : (c + 1) * width].reshape(bands * rows, width)

    @pl.when(is_reducer)
    def _():
        m_all = inbox_m.at[pl.ds(0, bands - 1)]
        pltpu.make_async_copy(m_all, m_all, m_recv).wait()
        own_rows = pl.ds(pl.multiple_of(number * rows, rows), rows)
        inbox_m[twin] = dense_ref[own_rows, :]
        inbox_p[me] = pdense[own_rows, :]
        left = inbox_m[...].astype(F32)
        row_id = lax.broadcasted_iota(jnp.int32, (rows, 2 * width), 0) + number * rows
        lane_id = lax.broadcasted_iota(jnp.int32, (rows, 2 * width), 1)
        row_f = (row_id - (radius - 1)).astype(F32)
        lane_g = (jnp.where(lane_id >= width, lane_id - width, lane_id) - (radius - 1)).astype(F32)
        kin = (row_f * row_f + lane_g * lane_g) * (1.0 / float(radius * radius))
        right = left * kin[None]
        keep(left_f, left)

        def overlaps(source):
            result = jnp.zeros((2 * bands, bands), F32)
            for r in range(rows):
                every = pl.ds(r, bands, stride=rows)
                low = jnp.concatenate([left_f[0, every, :], left_f[1, every, :]], axis=1)
                high_re, high_im = source[0, every, :], source[1, every, :]
                stack = jnp.concatenate(
                    [
                        jnp.concatenate([high_re, high_im], axis=1),
                        jnp.concatenate([-high_im, high_re], axis=1),
                    ],
                    axis=0,
                )
                result += dot_nt(stack.astype(BF16), low.astype(BF16))
            return result * (1.0 / float(4 * radius * radius))

        corr = overlaps(left_f)
        p_all = inbox_p.at[pl.ds(0, total - 1)]
        pltpu.make_async_copy(p_all, p_all, p_recv).wait()
        for g in range(groups):
            right += inbox_p[g * bands : (g + 1) * bands].astype(F32)
        keep(right_f, right)
        result = jnp.concatenate([overlaps(right_f), corr], axis=0)
        depth = message.shape[0]
        message[...] = jnp.concatenate(
            [result[f : f + depth] for f in range(0, 4 * bands, depth)], axis=1
        )
        inbox_s[number] = message[...]
        b_each(lambda copy: copy.start())

    for g in range(groups):
        arrived(got, x_recv, g)
    mine = got[0]
    for g in range(1, groups):
        mine += got[g]
    a_re = take_lanes(mine[:, :width], own_index)
    a_im = take_lanes(mine[:, width:], own_index)
    out_ref[0, 0] = jnp.where(present, kinetic * re + a_re, 0.0).astype(BF16)
    out_ref[1, 0] = jnp.where(present, kinetic * im + a_im, 0.0).astype(BF16)

    for copy in m_copies + p_copies + x_copies:
        copy.wait_send()

    @pl.when(is_reducer)
    def _():
        most = inbox_s.at[pl.ds(0, reducers - 1)]
        pltpu.make_async_copy(most, most, b_recv).wait()

    beside = (offset + 1 >= 0) & (offset + 1 < 2 * per_group) & (lax.rem(band, 2) == 0)

    @pl.when(beside)
    def _():
        pltpu.make_async_copy(inbox_m.at[0], inbox_m.at[0], m_recv).wait()
        pltpu.make_async_copy(inbox_p.at[0], inbox_p.at[0], p_recv).wait()

    @pl.when(jnp.logical_not(is_reducer))
    def _():
        pltpu.make_async_copy(inbox_s, inbox_s, b_recv).wait()

    final = inbox_s[0]
    for r in range(1, reducers):
        final += inbox_s[r]
    final = jnp.concatenate(
        [final[:, f : f + bands] for f in range(0, final.shape[1], bands)], axis=0
    )
    red_ref[0] = final[:bands]
    red_ref[1] = final[bands : 2 * bands]
    corr_ref[0] = final[2 * bands : 3 * bands]
    corr_ref[1] = final[3 * bands :]


    @pl.when(is_reducer)
    def _():
        b_each(lambda copy: copy.wait_send())


def write_out(out_ref, corr_ref, red_ref, out_hbm, corr_hbm, red_hbm, sem):
    copies = [
        pltpu.make_async_copy(out_ref, out_hbm, sem.at[0]),
        pltpu.make_async_copy(corr_ref, corr_hbm, sem.at[1]),
        pltpu.make_async_copy(red_ref, red_hbm, sem.at[2]),
    ]
    for copy in copies:
        copy.start()
    for copy in copies:
        copy.wait()


def body(bands, groups, orbitals, potential, slot_sticks, stick_entries):
    points = potential.shape[1]
    planes = potential.shape[0]
    width = stick_entries.shape[1]
    radius = width // 2
    slots = orbitals.shape[2]
    plane_pad = -(-planes // 128) * 128
    coarse = 2 * width
    reducers = width // 16
    per_group = reducers // groups
    rows = width // reducers
    fold = max(1, 128 // bands)
    slot_lanes = -(-groups * slots // 128) * 128
    tz, tb, tx, ty, tr = tables(points, width, radius, groups, planes, plane_pad, coarse)
    vmem = pl.BlockSpec(memory_space=pltpu.VMEM)
    hbm = pl.BlockSpec(memory_space=pltpu.HBM)
    total = bands * groups
    dma = pltpu.SemaphoreType.DMA
    results = pl.pallas_call(
        functools.partial(kernel, bands, groups, points, radius),
        out_shape=(
            pltpu.VMEM(orbitals.shape, BF16),
            pltpu.VMEM((2, bands, bands), F32),
            pltpu.VMEM((2, bands, bands), F32),
        ),
        in_specs=[hbm] * 9,
        out_specs=(vmem, vmem, vmem),
        scratch_shapes=[
            pltpu.VMEM(orbitals.shape, BF16),
            pltpu.VMEM(slot_sticks.shape, jnp.int32),
            pltpu.VMEM(stick_entries.shape, jnp.int32),
            pltpu.VMEM(tz.shape[1:], BF16),
            pltpu.VMEM(tb.shape[1:], BF16),
            pltpu.VMEM(tx.shape, BF16),
            pltpu.VMEM(ty.shape, BF16),
            pltpu.VMEM(tr.shape, BF16),
            pltpu.VMEM((plane_pad, points), F32),
            pltpu.VMEM((width, slot_lanes), F32),
            pltpu.VMEM((groups, slots, width), jnp.int32),
            pltpu.VMEM((groups, 2, slots, width), BF16),
            pltpu.VMEM((groups, slots, 2 * width), BF16),
            pltpu.VMEM((groups, slots, 2 * width), F32),
            pltpu.VMEM((groups, slots, 2 * width), F32),
            pltpu.VMEM((width, 2 * width), BF16),
            pltpu.VMEM((width, 2 * width), BF16),
            pltpu.VMEM((bands, rows, 2 * width), BF16),
            pltpu.VMEM((total, rows, 2 * width), BF16),
            pltpu.VMEM((2, bands * rows, width), F32),
            pltpu.VMEM((2, bands * rows, width), F32),
            pltpu.VMEM((4 * bands // fold, bands * fold), F32),
            pltpu.VMEM((reducers, 4 * bands // fold, bands * fold), F32),
            dma((9,)),
            pltpu.SemaphoreType.REGULAR((3,)),
            pltpu.SemaphoreType.REGULAR,
            dma((groups,)),
            dma((groups,)),
            dma((groups,)),
            dma((groups,)),
            dma((per_group,)),
            dma,
            dma((reducers,)),
            dma,
            dma((total,)),
            dma,
        ],
        compiler_params=pltpu.CompilerParams(
            collective_id=0, has_side_effects=True, vmem_limit_bytes=60000000
        ),
    )(orbitals, slot_sticks, stick_entries, potential, tz, tb, tx, ty, tr)
    return pl.pallas_call(
        write_out,
        out_shape=[jax.ShapeDtypeStruct(r.shape, r.dtype) for r in results],
        in_specs=[vmem] * 3,
        out_specs=[hbm] * 3,
        scratch_shapes=[dma((3,))],
    )(*[pltpu.with_memory_space_constraint(r, pltpu.VMEM) for r in results])


def solution(mesh):
    bands = mesh.shape["band"]
    groups = mesh.shape["ga"]
    return jax.shard_map(
        functools.partial(body, bands, groups),
        mesh=mesh,
        in_specs=(P(None, "band", "ga", None), P("ga", None), P(), P()),
        out_specs=(P(None, "band", "ga", None), P(), P()),
        check_vma=False,
    )
```

```python
import functools
import math

import jax
import jax.numpy as jnp
import numpy as np
from jax import lax
from jax.experimental import pallas as pl
from jax.experimental.pallas import tpu as pltpu
from jax.sharding import PartitionSpec as P

MESH = pl.DeviceIdType.MESH
NT = (((1,), (1,)), ((), ()))
BF16 = jnp.bfloat16
F32 = jnp.float32
BLOCK = 4
UNROLL = 8


def split_np(table):
    high = table.astype(np.float32).astype(BF16)
    low = (table - high.astype(np.float64)).astype(np.float32).astype(BF16)
    return np.stack([high, low])


def tables(points, width, radius, groups, planes, plane_pad, coarse):
    freq = np.arange(width) - radius + 1
    used = (np.arange(width) < width - 1).astype(np.float64)
    z_tabs = []
    for group in range(groups):
        z = np.arange(planes) + group * planes
        angle = 2.0 * np.pi * ((freq[:, None] * z[None, :]) % points) / points
        cos = np.zeros((width, plane_pad))
        sin = np.zeros((width, plane_pad))
        cos[:, :planes] = np.cos(angle) * used[:, None]
        sin[:, :planes] = np.sin(angle) * used[:, None]
        z_tabs.append(split_np(np.block([[cos, sin], [-sin, cos]])))
    x = np.arange(coarse)
    angle = 2.0 * np.pi * ((freq[None, :] * x[:, None]) % coarse) / coarse
    cos = np.cos(angle) * used[None, :]
    sin = np.sin(angle) * used[None, :]
    forward = np.block([[cos, -sin], [sin, cos]])
    limit = 2 * (radius - 1)
    offset = (x[:, None] * points - np.arange(points)[None, :] * coarse) % (coarse * points)
    base = 2.0 * np.pi * offset / (coarse * points)
    resample = np.ones((coarse, points))
    for g in range(1, limit + 1):
        resample += 2.0 * np.cos(g * base)
    resample /= points
    z_tabs = np.stack(z_tabs)
    return (
        z_tabs,
        np.swapaxes(z_tabs, 2, 3).copy(),
        split_np(forward),
        split_np(forward.T.copy()),
        split_np(resample),
    )


def split(value):
    high = value.astype(BF16)
    low = (value - high.astype(F32)).astype(BF16)
    return high, low


def thirds(value, axis):
    high, low = split(value)
    return jnp.concatenate([high, low, high], axis=axis)


def dot(a, b):
    return jnp.dot(a, b, preferred_element_type=F32)


def dot_nt(a, b):
    return lax.dot_general(a, b, NT, preferred_element_type=F32)


def take_lanes(value, index):
    return jnp.take_along_axis(value, index, axis=1, mode="promise_in_bounds")


def kernel(
    bands,
    groups,
    points,
    radius,
    orb_hbm,
    slots_hbm,
    entries_hbm,
    pot_hbm,
    tz_hbm,
    tb_hbm,
    tx_hbm,
    ty_hbm,
    tr_hbm,
    out_ref,
    corr_ref,
    red_ref,
    orb_ref,
    slots_ref,
    entries_ref,
    tz,
    tb,
    tx,
    ty,
    tr,
    pot,
    ent_t,
    inv_ref,
    raw,
    spread,
    part,
    got,
    dense_ref,
    pdense,
    inbox_m,
    inbox_p,
    left_f,
    right_f,
    message,
    inbox_s,
    load_sem,
    near_sem,
    s_send,
    s_recv,
    x_send,
    x_recv,
    m_send,
    m_recv,
    p_send,
    p_recv,
    b_send,
    b_recv,
):
    band = lax.axis_index("band")
    ga = lax.axis_index("ga")
    total = bands * groups
    twin = band + 1 - 2 * lax.rem(band, 2)
    me = ga * bands + twin
    slots = orb_hbm.shape[2]
    width = orb_hbm.shape[3]
    planes = pot_hbm.shape[0]
    plane_pad = pot.shape[0]
    coarse = tx.shape[1] // 2
    reducers = inbox_s.shape[0]
    rows = width // reducers
    per_group = reducers // groups
    block = math.gcd(bands, BLOCK)
    blocks = bands // block
    place = lax.rem(band, block)
    base = band - place
    first_band = bands // 2 - per_group + 1

    loads = [
        pltpu.make_async_copy(entries_hbm, entries_ref, load_sem.at[5]),
        pltpu.make_async_copy(orb_hbm, orb_ref, load_sem.at[6]),
        pltpu.make_async_copy(slots_hbm, slots_ref, load_sem.at[7]),
        pltpu.make_async_copy(pot_hbm, pot.at[pl.ds(0, planes)], load_sem.at[0]),
        pltpu.make_async_copy(tr_hbm, tr, load_sem.at[1]),
        pltpu.make_async_copy(tz_hbm.at[ga], tz, load_sem.at[2]),
        pltpu.make_async_copy(tx_hbm, tx, load_sem.at[3]),
        pltpu.make_async_copy(ty_hbm, ty, load_sem.at[4]),
        pltpu.make_async_copy(tb_hbm.at[ga], tb, load_sem.at[8]),
    ]
    load_entries, load_orb, load_slots, load_pot, load_tr, load_tz, load_tx, load_ty, load_tb = loads
    load_orb.start()

    has_low = band >= block
    has_high = band < bands - block
    barrier = pltpu.get_barrier_semaphore()
    across = band + 2 - 4 * lax.rem(lax.div(band, 2), 2)

    def greet(to_band, to_ga, semaphore=barrier):
        pl.semaphore_signal(semaphore, inc=1, device_id=(to_band, to_ga), device_id_type=MESH)

    for k in range(1, groups):
        greet(twin, lax.rem(ga + k, groups))
        greet(band, lax.rem(ga + k, groups))
    greet(twin, ga)
    greet(across, ga)

    def near(semaphore_low, semaphore_high):
        @pl.when(has_low)
        def _():
            pl.semaphore_signal(
                semaphore_high, inc=1, device_id=(band - block, ga), device_id_type=MESH
            )

        @pl.when(has_high)
        def _():
            pl.semaphore_signal(
                semaphore_low, inc=1, device_id=(band + block, ga), device_id_type=MESH
            )

    def near_wait():
        @pl.when(has_low)
        def _():
            pl.semaphore_wait(near_sem.at[0], 1)

        @pl.when(has_high)
        def _():
            pl.semaphore_wait(near_sem.at[1], 1)

    near(barrier, barrier)
    for load in loads:
        if load is not load_orb:
            load.start()
    if plane_pad > planes:
        pot[pl.ds(planes, plane_pad - planes), :] = jnp.zeros(
            (plane_pad - planes, pot.shape[1]), F32
        )

    load_orb.wait()
    pl.semaphore_wait(
        barrier, 2 * groups + has_low.astype(jnp.int32) + has_high.astype(jnp.int32)
    )
    s_copies = []
    for k in range(1, groups + 1):
        copy = pltpu.make_async_remote_copy(
            src_ref=orb_ref.at[:, 0],
            dst_ref=raw.at[ga],
            send_sem=s_send.at[k - 1],
            recv_sem=s_recv.at[ga],
            device_id=(twin, lax.rem(ga + k, groups)),
            device_id_type=MESH,
        )
        copy.start()
        s_copies.append(copy)

    def arrived(ref, sem, g):
        pltpu.make_async_copy(ref.at[g], ref.at[g], sem.at[g]).wait()

    greet(across, ga, near_sem.at[2])

    load_entries.wait()
    load_slots.wait()
    all_slots = groups * slots
    listed = entries_ref[...].astype(F32)
    slot_pad = ent_t.shape[1] - all_slots
    if slot_pad:
        listed = jnp.concatenate([listed, jnp.full((slot_pad, width), -1.0, F32)], axis=0)
    ent_t[...] = listed.T
    lanes = ent_t.shape[1]
    which = lax.broadcasted_iota(jnp.int32, (width, lanes), 0).astype(F32).astype(BF16)

    def invert(step, found):
        for u in range(UNROLL):
            k = step * UNROLL + u
            row = jnp.broadcast_to(ent_t[pl.ds(k, 1), :], (16, lanes)).astype(BF16)
            row = jnp.concatenate([row] * (width // 16), axis=0)
            found = jnp.where(row == which, k.astype(F32).astype(BF16), found)
        return found

    found = lax.fori_loop(
        0, width // UNROLL, invert, jnp.full((width, lanes), -1.0, BF16)
    )
    found = found.astype(F32).T.astype(jnp.int32)
    for g in range(groups):
        inv_ref[g] = found[g * slots : (g + 1) * slots]

    def spread_of(g):
        arrived(raw, s_recv, g)
        re = raw[g, 0].astype(F32)
        im = raw[g, 1].astype(F32)
        inverse = inv_ref[g]
        filled = inverse >= 0
        index = jnp.maximum(inverse, 0)
        spread[g, :, :width] = jnp.where(filled, take_lanes(re, index), 0.0).astype(BF16)
        spread[g, :, width:] = jnp.where(filled, take_lanes(im, index), 0.0).astype(BF16)

    re = orb_ref[0, 0].astype(F32)
    im = orb_ref[1, 0].astype(F32)
    spread_of(ga)

    rounds = max(blocks // 2, 1)
    pl.semaphore_wait(near_sem.at[2], 1)
    near(near_sem.at[0], near_sem.at[1])

    load_pot.wait()
    load_tr.wait()
    pot_hi, pot_lo = split(pot[...])
    weight = dot_nt(tr[0], pot_hi) + dot_nt(tr[0], pot_lo) + dot_nt(tr[1], pot_hi)

    near_wait()
    if rounds > 1:
        near(near_sem.at[0], near_sem.at[1])

    for k in range(1, groups):
        spread_of(lax.rem(ga + k, groups))
    for copy in s_copies:
        copy.wait_send()
    all_sticks = slots_ref[...].reshape(1, all_slots)
    sticks = [all_sticks[:, g * slots : (g + 1) * slots] for g in range(groups)]
    dense = jnp.zeros((width, 2 * width), F32)
    sub = lax.broadcasted_iota(jnp.int32, (width, slots), 0)
    for g in range(groups):
        choose = jnp.where(sub == sticks[g], 1.0, 0.0).astype(BF16)
        dense += dot(choose, spread[g])
    dense = dense.astype(BF16)
    dense_ref[...] = dense

    load_tz.wait()
    pair = jnp.concatenate([dense, dense], axis=1)
    z_table = jnp.concatenate([tz[0], tz[1]], axis=0)
    columns = [dot(pair, z_table[:, :plane_pad]), dot(pair, z_table[:, plane_pad:])]
    columns = jnp.concatenate(columns, axis=0)
    load_tx.wait()
    x_table = jnp.concatenate([tx[0], tx[0], tx[1]], axis=1)
    columns = thirds(columns, 0)
    quarter = coarse // 2
    field = jnp.concatenate(
        [dot(x_table[i * quarter : (i + 1) * quarter], columns) for i in range(4)], axis=0
    )
    product = jnp.concatenate([field[:coarse] * weight, field[coarse:] * weight], axis=0)
    product = thirds(product, 0)
    for r in range(1, rounds):
        near_wait()
        if r < rounds - 1:
            near(near_sem.at[0], near_sem.at[1])

    def place_of(r):
        return first_band + 2 * lax.rem(r, per_group), lax.div(r, per_group)

    def other(to_band, to_ga):
        own = (to_band == band) & (to_ga == ga)
        return jnp.where(own, band - 1, to_band), to_ga

    m_copies = []
    for q in range(per_group):
        start = pl.multiple_of((ga * per_group + q) * rows, rows)
        m_copies.append(
            pltpu.make_async_remote_copy(
                src_ref=dense_ref.at[pl.ds(start, rows)],
                dst_ref=inbox_m.at[twin],
                send_sem=m_send.at[q],
                recv_sem=m_recv,
                device_id=other(first_band + 2 * q, ga),
                device_id_type=MESH,
            )
        )
        m_copies[-1].start()

    load_ty.wait()
    y_table = jnp.concatenate([ty[0], ty[0], ty[1]], axis=1)
    back = jnp.concatenate([dot(y_table[:width], product), dot(y_table[width:], product)], axis=0)
    back = thirds(jnp.concatenate([back[:width], back[width:]], axis=1), 1)
    load_tb.wait()
    spectra = dot(back, jnp.concatenate([tb[0], tb[0], tb[1]], axis=0))
    spectra = spectra * (1.0 / float(points * coarse))
    spec_hi, spec_lo = split(spectra)
    pdense[...] = spec_hi

    nearest = jnp.where(
        band >= bands // 2, per_group // 2 + lax.div(lax.rem(band, block), 2), lax.div(lax.rem(band, block), 2)
    )
    nearest = lax.rem(nearest, per_group)

    def far_reducer(far):
        g = lax.rem(ga + far // per_group, groups)
        q, bit = 0, 1
        while bit < per_group:
            own_bit = lax.rem(lax.div(nearest, bit), 2)
            q = q + bit * (1 - own_bit if far % per_group & bit else own_bit)
            bit *= 2
        return g * per_group + q

    p_copies = []
    for far in reversed(range(reducers)):
        r = far_reducer(far)
        p_copies.append(
            pltpu.make_async_remote_copy(
                src_ref=pdense.at[pl.ds(pl.multiple_of(r * rows, rows), rows)],
                dst_ref=inbox_p.at[me],
                send_sem=p_send.at[far],
                recv_sem=p_recv,
                device_id=other(*place_of(r)),
                device_id_type=MESH,
            )
        )
        p_copies[-1].start()

    eye = lax.broadcasted_iota(jnp.int32, (slots, slots), 0) == lax.broadcasted_iota(
        jnp.int32, (slots, slots), 1
    )

    def stick_column(g):
        row = sticks[0]
        for other in range(1, groups):
            row = jnp.where(g == other, sticks[other], row)
        row = row.astype(F32)
        return jnp.sum(jnp.where(eye, row, 0.0), axis=1, keepdims=True)

    lane = lax.broadcasted_iota(jnp.int32, (slots, width), 1)
    lane_f = lane.astype(F32)
    x_copies = []
    for k in range(1, groups + 1):
        target = lax.rem(ga + k, groups)
        stick = stick_column(target)
        choose = jnp.where(stick == lane_f, 1.0, 0.0).astype(BF16)
        mine = dot(choose, spec_hi) + dot(choose, spec_lo)
        part[k - 1] = mine
        x_copies.append(
            pltpu.make_async_remote_copy(
                src_ref=part.at[k - 1],
                dst_ref=got.at[ga],
                send_sem=x_send.at[k - 1],
                recv_sem=x_recv.at[ga],
                device_id=(twin, target),
                device_id_type=MESH,
            )
        )

    own = entries_ref[pl.ds(pl.multiple_of(ga * slots, 8), slots)]
    present = own >= 0
    gx = stick - float(radius - 1)
    gz = (own - (radius - 1)).astype(F32)
    kinetic = (gx * gx + gz * gz) * (1.0 / float(radius * radius))
    own_index = jnp.maximum(own, 0)

    for copy in x_copies:
        copy.start()

    offset = band - first_band
    is_reducer = (offset >= 0) & (offset < 2 * per_group) & (lax.rem(band + 1, 2) == 0)
    number = ga * per_group + lax.div(jnp.clip(offset, 0, 2 * per_group - 1), 2)

    order = band * groups + ga

    def b_copy(t):
        if isinstance(t, int):
            to_band, to_ga = t // groups, t % groups
        else:
            to_band, to_ga = lax.div(t, groups), lax.rem(t, groups)
        return pltpu.make_async_remote_copy(
            src_ref=message,
            dst_ref=inbox_s.at[number],
            send_sem=b_send.at[t],
            recv_sem=b_recv,
            device_id=(to_band, to_ga),
            device_id_type=MESH,
        )

    def b_each(act):
        if total <= 64:
            for t in range(total):

                @pl.when(order != t)
                def _(t=t):
                    act(b_copy(t))
        else:

            @pl.loop(0, total)
            def _(t):
                @pl.when(order != t)
                def _():
                    act(b_copy(t))

    def keep(ref, value):
        for c in range(2):
            ref[c] = value[:, :, c * width : (c + 1) * width].reshape(bands * rows, width)

    @pl.when(is_reducer)
    def _():
        m_all = inbox_m.at[pl.ds(0, bands - 1)]
        pltpu.make_async_copy(m_all, m_all, m_recv).wait()
        own_rows = pl.ds(pl.multiple_of(number * rows, rows), rows)
        inbox_m[twin] = dense_ref[own_rows, :]
        inbox_p[me] = pdense[own_rows, :]
        left = inbox_m[...].astype(F32)
        row_id = lax.broadcasted_iota(jnp.int32, (rows, 2 * width), 0) + number * rows
        lane_id = lax.broadcasted_iota(jnp.int32, (rows, 2 * width), 1)
        row_f = (row_id - (radius - 1)).astype(F32)
        lane_g = (jnp.where(lane_id >= width, lane_id - width, lane_id) - (radius - 1)).astype(F32)
        kin = (row_f * row_f + lane_g * lane_g) * (1.0 / float(radius * radius))
        right = left * kin[None]
        keep(left_f, left)

        def overlaps(source):
            result = jnp.zeros((2 * bands, bands), F32)
            for r in range(rows):
                every = pl.ds(r, bands, stride=rows)
                low = jnp.concatenate([left_f[0, every, :], left_f[1, every, :]], axis=1)
                high_re, high_im = source[0, every, :], source[1, every, :]
                stack = jnp.concatenate(
                    [
                        jnp.concatenate([high_re, high_im], axis=1),
                        jnp.concatenate([-high_im, high_re], axis=1),
                    ],
                    axis=0,
                )
                result += dot_nt(stack.astype(BF16), low.astype(BF16))
            return result * (1.0 / float(4 * radius * radius))

        corr = overlaps(left_f)
        p_all = inbox_p.at[pl.ds(0, total - 1)]
        pltpu.make_async_copy(p_all, p_all, p_recv).wait()
        for g in range(groups):
            right += inbox_p[g * bands : (g + 1) * bands].astype(F32)
        keep(right_f, right)
        result = jnp.concatenate([overlaps(right_f), corr], axis=0)
        depth = message.shape[0]
        message[...] = jnp.concatenate(
            [result[f : f + depth] for f in range(0, 4 * bands, depth)], axis=1
        )
        inbox_s[number] = message[...]
        b_each(lambda copy: copy.start())

    for g in range(groups):
        arrived(got, x_recv, g)
    mine = got[0]
    for g in range(1, groups):
        mine += got[g]
    a_re = take_lanes(mine[:, :width], own_index)
    a_im = take_lanes(mine[:, width:], own_index)
    out_ref[0, 0] = jnp.where(present, kinetic * re + a_re, 0.0).astype(BF16)
    out_ref[1, 0] = jnp.where(present, kinetic * im + a_im, 0.0).astype(BF16)

    for copy in m_copies + p_copies + x_copies:
        copy.wait_send()

    @pl.when(is_reducer)
    def _():
        most = inbox_s.at[pl.ds(0, reducers - 1)]
        pltpu.make_async_copy(most, most, b_recv).wait()

    beside = (offset + 1 >= 0) & (offset + 1 < 2 * per_group) & (lax.rem(band, 2) == 0)

    @pl.when(beside)
    def _():
        pltpu.make_async_copy(inbox_m.at[0], inbox_m.at[0], m_recv).wait()
        pltpu.make_async_copy(inbox_p.at[0], inbox_p.at[0], p_recv).wait()

    @pl.when(jnp.logical_not(is_reducer))
    def _():
        pltpu.make_async_copy(inbox_s, inbox_s, b_recv).wait()

    final = inbox_s[0]
    for r in range(1, reducers):
        final += inbox_s[r]
    final = jnp.concatenate(
        [final[:, f : f + bands] for f in range(0, final.shape[1], bands)], axis=0
    )
    red_ref[0] = final[:bands]
    red_ref[1] = final[bands : 2 * bands]
    corr_ref[0] = final[2 * bands : 3 * bands]
    corr_ref[1] = final[3 * bands :]


    @pl.when(is_reducer)
    def _():
        b_each(lambda copy: copy.wait_send())


def write_out(out_ref, corr_ref, red_ref, out_hbm, corr_hbm, red_hbm, sem):
    copies = [
        pltpu.make_async_copy(out_ref, out_hbm, sem.at[0]),
        pltpu.make_async_copy(corr_ref, corr_hbm, sem.at[1]),
        pltpu.make_async_copy(red_ref, red_hbm, sem.at[2]),
    ]
    for copy in copies:
        copy.start()
    for copy in copies:
        copy.wait()


def body(bands, groups, orbitals, potential, slot_sticks, stick_entries):
    points = potential.shape[1]
    planes = potential.shape[0]
    width = stick_entries.shape[1]
    radius = width // 2
    slots = orbitals.shape[2]
    plane_pad = -(-planes // 128) * 128
    coarse = 2 * width
    reducers = width // 16
    per_group = reducers // groups
    rows = width // reducers
    fold = max(1, 128 // bands)
    slot_lanes = -(-groups * slots // 128) * 128
    tz, tb, tx, ty, tr = tables(points, width, radius, groups, planes, plane_pad, coarse)
    vmem = pl.BlockSpec(memory_space=pltpu.VMEM)
    hbm = pl.BlockSpec(memory_space=pltpu.HBM)
    total = bands * groups
    dma = pltpu.SemaphoreType.DMA
    results = pl.pallas_call(
        functools.partial(kernel, bands, groups, points, radius),
        out_shape=(
            pltpu.VMEM(orbitals.shape, BF16),
            pltpu.VMEM((2, bands, bands), F32),
            pltpu.VMEM((2, bands, bands), F32),
        ),
        in_specs=[hbm] * 9,
        out_specs=(vmem, vmem, vmem),
        scratch_shapes=[
            pltpu.VMEM(orbitals.shape, BF16),
            pltpu.VMEM(slot_sticks.shape, jnp.int32),
            pltpu.VMEM(stick_entries.shape, jnp.int32),
            pltpu.VMEM(tz.shape[1:], BF16),
            pltpu.VMEM(tb.shape[1:], BF16),
            pltpu.VMEM(tx.shape, BF16),
            pltpu.VMEM(ty.shape, BF16),
            pltpu.VMEM(tr.shape, BF16),
            pltpu.VMEM((plane_pad, points), F32),
            pltpu.VMEM((width, slot_lanes), F32),
            pltpu.VMEM((groups, slots, width), jnp.int32),
            pltpu.VMEM((groups, 2, slots, width), BF16),
            pltpu.VMEM((groups, slots, 2 * width), BF16),
            pltpu.VMEM((groups, slots, 2 * width), F32),
            pltpu.VMEM((groups, slots, 2 * width), F32),
            pltpu.VMEM((width, 2 * width), BF16),
            pltpu.VMEM((width, 2 * width), BF16),
            pltpu.VMEM((bands, rows, 2 * width), BF16),
            pltpu.VMEM((total, rows, 2 * width), BF16),
            pltpu.VMEM((2, bands * rows, width), F32),
            pltpu.VMEM((2, bands * rows, width), F32),
            pltpu.VMEM((4 * bands // fold, bands * fold), F32),
            pltpu.VMEM((reducers, 4 * bands // fold, bands * fold), F32),
            dma((9,)),
            pltpu.SemaphoreType.REGULAR((3,)),
            dma((groups,)),
            dma((groups,)),
            dma((groups,)),
            dma((groups,)),
            dma((per_group,)),
            dma,
            dma((reducers,)),
            dma,
            dma((total,)),
            dma,
        ],
        compiler_params=pltpu.CompilerParams(
            collective_id=0, has_side_effects=True, vmem_limit_bytes=60000000
        ),
    )(orbitals, slot_sticks, stick_entries, potential, tz, tb, tx, ty, tr)
    return pl.pallas_call(
        write_out,
        out_shape=[jax.ShapeDtypeStruct(r.shape, r.dtype) for r in results],
        in_specs=[vmem] * 3,
        out_specs=[hbm] * 3,
        scratch_shapes=[dma((3,))],
    )(*[pltpu.with_memory_space_constraint(r, pltpu.VMEM) for r in results])


def solution(mesh):
    bands = mesh.shape["band"]
    groups = mesh.shape["ga"]
    return jax.shard_map(
        functools.partial(body, bands, groups),
        mesh=mesh,
        in_specs=(P(None, "band", "ga", None), P("ga", None), P(), P()),
        out_specs=(P(None, "band", "ga", None), P(), P()),
        check_vma=False,
    )
```

```python
import functools
import math

import jax
import jax.numpy as jnp
import numpy as np
from jax import lax
from jax.experimental import pallas as pl
from jax.experimental.pallas import tpu as pltpu
from jax.sharding import PartitionSpec as P

MESH = pl.DeviceIdType.MESH
NT = (((1,), (1,)), ((), ()))
BF16 = jnp.bfloat16
F32 = jnp.float32
BLOCK = 4
UNROLL = 8


def split_np(table):
    high = table.astype(np.float32).astype(BF16)
    low = (table - high.astype(np.float64)).astype(np.float32).astype(BF16)
    return np.stack([high, low])


def tables(points, width, radius, groups, planes, plane_pad, coarse):
    freq = np.arange(width) - radius + 1
    used = (np.arange(width) < width - 1).astype(np.float64)
    z_tabs = []
    for group in range(groups):
        z = np.arange(planes) + group * planes
        angle = 2.0 * np.pi * ((freq[:, None] * z[None, :]) % points) / points
        cos = np.zeros((width, plane_pad))
        sin = np.zeros((width, plane_pad))
        cos[:, :planes] = np.cos(angle) * used[:, None]
        sin[:, :planes] = np.sin(angle) * used[:, None]
        z_tabs.append(split_np(np.block([[cos, sin], [-sin, cos]])))
    x = np.arange(coarse)
    angle = 2.0 * np.pi * ((freq[None, :] * x[:, None]) % coarse) / coarse
    cos = np.cos(angle) * used[None, :]
    sin = np.sin(angle) * used[None, :]
    forward = np.block([[cos, -sin], [sin, cos]])
    limit = 2 * (radius - 1)
    offset = (x[:, None] * points - np.arange(points)[None, :] * coarse) % (coarse * points)
    base = 2.0 * np.pi * offset / (coarse * points)
    resample = np.ones((coarse, points))
    for g in range(1, limit + 1):
        resample += 2.0 * np.cos(g * base)
    resample /= points
    z_tabs = np.stack(z_tabs)
    return (
        z_tabs,
        np.swapaxes(z_tabs, 2, 3).copy(),
        split_np(forward),
        split_np(forward.T.copy()),
        split_np(resample),
    )


def split(value):
    high = value.astype(BF16)
    low = (value - high.astype(F32)).astype(BF16)
    return high, low


def thirds(value, axis):
    high, low = split(value)
    return jnp.concatenate([high, low, high], axis=axis)


def dot(a, b):
    return jnp.dot(a, b, preferred_element_type=F32)


def dot_nt(a, b):
    return lax.dot_general(a, b, NT, preferred_element_type=F32)


def take_lanes(value, index):
    return jnp.take_along_axis(value, index, axis=1, mode="promise_in_bounds")


def kernel(
    bands,
    groups,
    points,
    radius,
    orb_hbm,
    slots_hbm,
    entries_hbm,
    pot_hbm,
    tz_hbm,
    tb_hbm,
    tx_hbm,
    ty_hbm,
    tr_hbm,
    out_ref,
    corr_ref,
    red_ref,
    orb_ref,
    slots_ref,
    entries_ref,
    tz,
    tb,
    tx,
    ty,
    tr,
    pot,
    ent_t,
    inv_ref,
    raw,
    spread,
    part,
    got,
    dense_ref,
    pdense,
    inbox_m,
    inbox_p,
    left_f,
    right_f,
    message,
    inbox_s,
    load_sem,
    near_sem,
    s_send,
    s_recv,
    x_send,
    x_recv,
    m_send,
    m_recv,
    p_send,
    p_recv,
    b_send,
    b_recv,
):
    band = lax.axis_index("band")
    ga = lax.axis_index("ga")
    total = bands * groups
    twin = band + 1 - 2 * lax.rem(band, 2)
    me = ga * bands + twin
    slots = orb_hbm.shape[2]
    width = orb_hbm.shape[3]
    planes = pot_hbm.shape[0]
    plane_pad = pot.shape[0]
    coarse = tx.shape[1] // 2
    reducers = inbox_s.shape[0]
    rows = width // reducers
    per_group = reducers // groups
    block = math.gcd(bands, BLOCK)
    blocks = bands // block
    place = lax.rem(band, block)
    base = band - place
    first_band = bands // 2 - per_group + 1

    loads = [
        pltpu.make_async_copy(entries_hbm, entries_ref, load_sem.at[5]),
        pltpu.make_async_copy(orb_hbm, orb_ref, load_sem.at[6]),
        pltpu.make_async_copy(slots_hbm, slots_ref, load_sem.at[7]),
        pltpu.make_async_copy(pot_hbm, pot.at[pl.ds(0, planes)], load_sem.at[0]),
        pltpu.make_async_copy(tr_hbm, tr, load_sem.at[1]),
        pltpu.make_async_copy(tz_hbm.at[ga], tz, load_sem.at[2]),
        pltpu.make_async_copy(tx_hbm, tx, load_sem.at[3]),
        pltpu.make_async_copy(ty_hbm, ty, load_sem.at[4]),
        pltpu.make_async_copy(tb_hbm.at[ga], tb, load_sem.at[8]),
    ]
    load_entries, load_orb, load_slots, load_pot, load_tr, load_tz, load_tx, load_ty, load_tb = loads
    load_orb.start()

    has_low = band >= block
    has_high = band < bands - block
    barrier = pltpu.get_barrier_semaphore()
    across = band + 2 - 4 * lax.rem(lax.div(band, 2), 2)

    def greet(to_band, to_ga, semaphore=barrier):
        pl.semaphore_signal(semaphore, inc=1, device_id=(to_band, to_ga), device_id_type=MESH)

    for k in range(1, groups):
        greet(twin, lax.rem(ga + k, groups))
        greet(band, lax.rem(ga + k, groups))
    greet(twin, ga)
    greet(across, ga)

    def near(semaphore_low, semaphore_high):
        @pl.when(has_low)
        def _():
            pl.semaphore_signal(
                semaphore_high, inc=1, device_id=(band - block, ga), device_id_type=MESH
            )

        @pl.when(has_high)
        def _():
            pl.semaphore_signal(
                semaphore_low, inc=1, device_id=(band + block, ga), device_id_type=MESH
            )

    def near_wait():
        @pl.when(has_low)
        def _():
            pl.semaphore_wait(near_sem.at[0], 1)

        @pl.when(has_high)
        def _():
            pl.semaphore_wait(near_sem.at[1], 1)

    near(barrier, barrier)
    for load in loads:
        if load is not load_orb:
            load.start()
    if plane_pad > planes:
        pot[pl.ds(planes, plane_pad - planes), :] = jnp.zeros(
            (plane_pad - planes, pot.shape[1]), F32
        )

    load_orb.wait()
    pl.semaphore_wait(
        barrier, 2 * groups + has_low.astype(jnp.int32) + has_high.astype(jnp.int32)
    )
    s_copies = []
    for k in range(1, groups + 1):
        copy = pltpu.make_async_remote_copy(
            src_ref=orb_ref.at[:, 0],
            dst_ref=raw.at[ga],
            send_sem=s_send.at[k - 1],
            recv_sem=s_recv.at[ga],
            device_id=(twin, lax.rem(ga + k, groups)),
            device_id_type=MESH,
        )
        copy.start()
        s_copies.append(copy)

    def arrived(ref, sem, g):
        pltpu.make_async_copy(ref.at[g], ref.at[g], sem.at[g]).wait()

    greet(across, ga, near_sem.at[2])

    load_entries.wait()
    load_slots.wait()
    all_slots = groups * slots
    listed = entries_ref[...].astype(F32)
    slot_pad = ent_t.shape[1] - all_slots
    if slot_pad:
        listed = jnp.concatenate([listed, jnp.full((slot_pad, width), -1.0, F32)], axis=0)
    ent_t[...] = listed.T
    lanes = ent_t.shape[1]
    which = lax.broadcasted_iota(jnp.int32, (width, lanes), 0).astype(F32).astype(BF16)

    def invert(step, found):
        for u in range(UNROLL):
            k = step * UNROLL + u
            row = jnp.broadcast_to(ent_t[pl.ds(k, 1), :], (16, lanes)).astype(BF16)
            row = jnp.concatenate([row] * (width // 16), axis=0)
            found = jnp.where(row == which, k.astype(F32).astype(BF16), found)
        return found

    found = lax.fori_loop(
        0, width // UNROLL, invert, jnp.full((width, lanes), -1.0, BF16)
    )
    found = found.astype(F32).T.astype(jnp.int32)
    for g in range(groups):
        inv_ref[g] = found[g * slots : (g + 1) * slots]

    def spread_of(g):
        arrived(raw, s_recv, g)
        re = raw[g, 0].astype(F32)
        im = raw[g, 1].astype(F32)
        inverse = inv_ref[g]
        filled = inverse >= 0
        index = jnp.maximum(inverse, 0)
        spread[g, :, :width] = jnp.where(filled, take_lanes(re, index), 0.0).astype(BF16)
        spread[g, :, width:] = jnp.where(filled, take_lanes(im, index), 0.0).astype(BF16)

    re = orb_ref[0, 0].astype(F32)
    im = orb_ref[1, 0].astype(F32)
    spread_of(ga)

    rounds = max(blocks // 2, 1)
    pl.semaphore_wait(near_sem.at[2], 1)
    near(near_sem.at[0], near_sem.at[1])

    load_pot.wait()
    load_tr.wait()
    pot_hi, pot_lo = split(pot[...])
    weight = dot_nt(tr[0], pot_hi) + dot_nt(tr[0], pot_lo) + dot_nt(tr[1], pot_hi)

    near_wait()
    if rounds > 1:
        near(near_sem.at[0], near_sem.at[1])

    all_sticks = slots_ref[...].reshape(1, all_slots)
    sticks = [all_sticks[:, g * slots : (g + 1) * slots] for g in range(groups)]
    sub = lax.broadcasted_iota(jnp.int32, (width, slots), 0)

    def chosen_of(g):
        row = sticks[0]
        for other_ga in range(1, groups):
            row = jnp.where(g == other_ga, sticks[other_ga], row)
        return jnp.where(sub == row, 1.0, 0.0).astype(BF16)

    chosen = [chosen_of(lax.rem(ga + k, groups)) for k in range(1, groups)]
    dense = dot(chosen_of(ga), spread[ga])

    for k in range(1, groups):
        spread_of(lax.rem(ga + k, groups))
    for copy in s_copies:
        copy.wait_send()
    for k in range(1, groups):
        dense += dot(chosen[k - 1], spread[lax.rem(ga + k, groups)])
    dense = dense.astype(BF16)
    dense_ref[...] = dense

    load_tz.wait()
    pair = jnp.concatenate([dense, dense], axis=1)
    z_table = jnp.concatenate([tz[0], tz[1]], axis=0)
    columns = [dot(pair, z_table[:, :plane_pad]), dot(pair, z_table[:, plane_pad:])]
    columns = jnp.concatenate(columns, axis=0)
    load_tx.wait()
    x_table = jnp.concatenate([tx[0], tx[0], tx[1]], axis=1)
    columns = thirds(columns, 0)
    quarter = coarse // 2
    field = jnp.concatenate(
        [dot(x_table[i * quarter : (i + 1) * quarter], columns) for i in range(4)], axis=0
    )
    product = jnp.concatenate([field[:coarse] * weight, field[coarse:] * weight], axis=0)
    product = thirds(product, 0)
    for r in range(1, rounds):
        near_wait()
        if r < rounds - 1:
            near(near_sem.at[0], near_sem.at[1])

    def place_of(r):
        return first_band + 2 * lax.rem(r, per_group), lax.div(r, per_group)

    def other(to_band, to_ga):
        own = (to_band == band) & (to_ga == ga)
        return jnp.where(own, band - 1, to_band), to_ga

    m_copies = []
    for q in range(per_group):
        start = pl.multiple_of((ga * per_group + q) * rows, rows)
        m_copies.append(
            pltpu.make_async_remote_copy(
                src_ref=dense_ref.at[pl.ds(start, rows)],
                dst_ref=inbox_m.at[twin],
                send_sem=m_send.at[q],
                recv_sem=m_recv,
                device_id=other(first_band + 2 * q, ga),
                device_id_type=MESH,
            )
        )
        m_copies[-1].start()

    load_ty.wait()
    y_table = jnp.concatenate([ty[0], ty[0], ty[1]], axis=1)
    back = jnp.concatenate([dot(y_table[:width], product), dot(y_table[width:], product)], axis=0)
    back = thirds(jnp.concatenate([back[:width], back[width:]], axis=1), 1)
    load_tb.wait()
    spectra = dot(back, jnp.concatenate([tb[0], tb[0], tb[1]], axis=0))
    spectra = spectra * (1.0 / float(points * coarse))
    spec_hi, spec_lo = split(spectra)
    pdense[...] = spec_hi

    nearest = jnp.where(
        band >= bands // 2, per_group // 2 + lax.div(lax.rem(band, block), 2), lax.div(lax.rem(band, block), 2)
    )
    nearest = lax.rem(nearest, per_group)

    def far_reducer(far):
        g = lax.rem(ga + far // per_group, groups)
        q, bit = 0, 1
        while bit < per_group:
            own_bit = lax.rem(lax.div(nearest, bit), 2)
            q = q + bit * (1 - own_bit if far % per_group & bit else own_bit)
            bit *= 2
        return g * per_group + q

    p_copies = []
    for far in reversed(range(reducers)):
        r = far_reducer(far)
        p_copies.append(
            pltpu.make_async_remote_copy(
                src_ref=pdense.at[pl.ds(pl.multiple_of(r * rows, rows), rows)],
                dst_ref=inbox_p.at[me],
                send_sem=p_send.at[far],
                recv_sem=p_recv,
                device_id=other(*place_of(r)),
                device_id_type=MESH,
            )
        )
        p_copies[-1].start()

    eye = lax.broadcasted_iota(jnp.int32, (slots, slots), 0) == lax.broadcasted_iota(
        jnp.int32, (slots, slots), 1
    )

    def stick_column(g):
        row = sticks[0]
        for other in range(1, groups):
            row = jnp.where(g == other, sticks[other], row)
        row = row.astype(F32)
        return jnp.sum(jnp.where(eye, row, 0.0), axis=1, keepdims=True)

    lane = lax.broadcasted_iota(jnp.int32, (slots, width), 1)
    lane_f = lane.astype(F32)
    x_copies = []
    for k in range(1, groups + 1):
        target = lax.rem(ga + k, groups)
        stick = stick_column(target)
        choose = jnp.where(stick == lane_f, 1.0, 0.0).astype(BF16)
        mine = dot(choose, spec_hi) + dot(choose, spec_lo)
        part[k - 1] = mine
        x_copies.append(
            pltpu.make_async_remote_copy(
                src_ref=part.at[k - 1],
                dst_ref=got.at[ga],
                send_sem=x_send.at[k - 1],
                recv_sem=x_recv.at[ga],
                device_id=(twin, target),
                device_id_type=MESH,
            )
        )

    own = entries_ref[pl.ds(pl.multiple_of(ga * slots, 8), slots)]
    present = own >= 0
    gx = stick - float(radius - 1)
    gz = (own - (radius - 1)).astype(F32)
    kinetic = (gx * gx + gz * gz) * (1.0 / float(radius * radius))
    own_index = jnp.maximum(own, 0)

    for copy in x_copies:
        copy.start()

    offset = band - first_band
    is_reducer = (offset >= 0) & (offset < 2 * per_group) & (lax.rem(band + 1, 2) == 0)
    number = ga * per_group + lax.div(jnp.clip(offset, 0, 2 * per_group - 1), 2)

    order = band * groups + ga

    def b_copy(t):
        if isinstance(t, int):
            to_band, to_ga = t // groups, t % groups
        else:
            to_band, to_ga = lax.div(t, groups), lax.rem(t, groups)
        return pltpu.make_async_remote_copy(
            src_ref=message,
            dst_ref=inbox_s.at[number],
            send_sem=b_send.at[t],
            recv_sem=b_recv,
            device_id=(to_band, to_ga),
            device_id_type=MESH,
        )

    def b_each(act):
        if total <= 64:
            for t in range(total):

                @pl.when(order != t)
                def _(t=t):
                    act(b_copy(t))
        else:

            @pl.loop(0, total)
            def _(t):
                @pl.when(order != t)
                def _():
                    act(b_copy(t))

    def keep(ref, value):
        for c in range(2):
            ref[c] = value[:, :, c * width : (c + 1) * width].reshape(bands * rows, width)

    @pl.when(is_reducer)
    def _():
        m_all = inbox_m.at[pl.ds(0, bands - 1)]
        pltpu.make_async_copy(m_all, m_all, m_recv).wait()
        own_rows = pl.ds(pl.multiple_of(number * rows, rows), rows)
        inbox_m[twin] = dense_ref[own_rows, :]
        inbox_p[me] = pdense[own_rows, :]
        left = inbox_m[...].astype(F32)
        row_id = lax.broadcasted_iota(jnp.int32, (rows, 2 * width), 0) + number * rows
        lane_id = lax.broadcasted_iota(jnp.int32, (rows, 2 * width), 1)
        row_f = (row_id - (radius - 1)).astype(F32)
        lane_g = (jnp.where(lane_id >= width, lane_id - width, lane_id) - (radius - 1)).astype(F32)
        kin = (row_f * row_f + lane_g * lane_g) * (1.0 / float(radius * radius))
        right = left * kin[None]
        keep(left_f, left)

        def overlaps(source):
            result = jnp.zeros((2 * bands, bands), F32)
            for r in range(rows):
                every = pl.ds(r, bands, stride=rows)
                low = jnp.concatenate([left_f[0, every, :], left_f[1, every, :]], axis=1)
                high_re, high_im = source[0, every, :], source[1, every, :]
                stack = jnp.concatenate(
                    [
                        jnp.concatenate([high_re, high_im], axis=1),
                        jnp.concatenate([-high_im, high_re], axis=1),
                    ],
                    axis=0,
                )
                result += dot_nt(stack.astype(BF16), low.astype(BF16))
            return result * (1.0 / float(4 * radius * radius))

        corr = overlaps(left_f)
        p_all = inbox_p.at[pl.ds(0, total - 1)]
        pltpu.make_async_copy(p_all, p_all, p_recv).wait()
        for g in range(groups):
            right += inbox_p[g * bands : (g + 1) * bands].astype(F32)
        keep(right_f, right)
        result = jnp.concatenate([overlaps(right_f), corr], axis=0)
        depth = message.shape[0]
        message[...] = jnp.concatenate(
            [result[f : f + depth] for f in range(0, 4 * bands, depth)], axis=1
        )
        inbox_s[number] = message[...]
        b_each(lambda copy: copy.start())

    for g in range(groups):
        arrived(got, x_recv, g)
    mine = got[0]
    for g in range(1, groups):
        mine += got[g]
    a_re = take_lanes(mine[:, :width], own_index)
    a_im = take_lanes(mine[:, width:], own_index)
    out_ref[0, 0] = jnp.where(present, kinetic * re + a_re, 0.0).astype(BF16)
    out_ref[1, 0] = jnp.where(present, kinetic * im + a_im, 0.0).astype(BF16)

    for copy in m_copies + p_copies + x_copies:
        copy.wait_send()

    @pl.when(is_reducer)
    def _():
        most = inbox_s.at[pl.ds(0, reducers - 1)]
        pltpu.make_async_copy(most, most, b_recv).wait()

    beside = (offset + 1 >= 0) & (offset + 1 < 2 * per_group) & (lax.rem(band, 2) == 0)

    @pl.when(beside)
    def _():
        pltpu.make_async_copy(inbox_m.at[0], inbox_m.at[0], m_recv).wait()
        pltpu.make_async_copy(inbox_p.at[0], inbox_p.at[0], p_recv).wait()

    @pl.when(jnp.logical_not(is_reducer))
    def _():
        pltpu.make_async_copy(inbox_s, inbox_s, b_recv).wait()

    final = inbox_s[0]
    for r in range(1, reducers):
        final += inbox_s[r]
    final = jnp.concatenate(
        [final[:, f : f + bands] for f in range(0, final.shape[1], bands)], axis=0
    )
    red_ref[0] = final[:bands]
    red_ref[1] = final[bands : 2 * bands]
    corr_ref[0] = final[2 * bands : 3 * bands]
    corr_ref[1] = final[3 * bands :]


    @pl.when(is_reducer)
    def _():
        b_each(lambda copy: copy.wait_send())


def write_out(out_ref, corr_ref, red_ref, out_hbm, corr_hbm, red_hbm, sem):
    copies = [
        pltpu.make_async_copy(out_ref, out_hbm, sem.at[0]),
        pltpu.make_async_copy(corr_ref, corr_hbm, sem.at[1]),
        pltpu.make_async_copy(red_ref, red_hbm, sem.at[2]),
    ]
    for copy in copies:
        copy.start()
    for copy in copies:
        copy.wait()


def body(bands, groups, orbitals, potential, slot_sticks, stick_entries):
    points = potential.shape[1]
    planes = potential.shape[0]
    width = stick_entries.shape[1]
    radius = width // 2
    slots = orbitals.shape[2]
    plane_pad = -(-planes // 128) * 128
    coarse = 2 * width
    reducers = width // 16
    per_group = reducers // groups
    rows = width // reducers
    fold = max(1, 128 // bands)
    slot_lanes = -(-groups * slots // 128) * 128
    tz, tb, tx, ty, tr = tables(points, width, radius, groups, planes, plane_pad, coarse)
    vmem = pl.BlockSpec(memory_space=pltpu.VMEM)
    hbm = pl.BlockSpec(memory_space=pltpu.HBM)
    total = bands * groups
    dma = pltpu.SemaphoreType.DMA
    results = pl.pallas_call(
        functools.partial(kernel, bands, groups, points, radius),
        out_shape=(
            pltpu.VMEM(orbitals.shape, BF16),
            pltpu.VMEM((2, bands, bands), F32),
            pltpu.VMEM((2, bands, bands), F32),
        ),
        in_specs=[hbm] * 9,
        out_specs=(vmem, vmem, vmem),
        scratch_shapes=[
            pltpu.VMEM(orbitals.shape, BF16),
            pltpu.VMEM(slot_sticks.shape, jnp.int32),
            pltpu.VMEM(stick_entries.shape, jnp.int32),
            pltpu.VMEM(tz.shape[1:], BF16),
            pltpu.VMEM(tb.shape[1:], BF16),
            pltpu.VMEM(tx.shape, BF16),
            pltpu.VMEM(ty.shape, BF16),
            pltpu.VMEM(tr.shape, BF16),
            pltpu.VMEM((plane_pad, points), F32),
            pltpu.VMEM((width, slot_lanes), F32),
            pltpu.VMEM((groups, slots, width), jnp.int32),
            pltpu.VMEM((groups, 2, slots, width), BF16),
            pltpu.VMEM((groups, slots, 2 * width), BF16),
            pltpu.VMEM((groups, slots, 2 * width), F32),
            pltpu.VMEM((groups, slots, 2 * width), F32),
            pltpu.VMEM((width, 2 * width), BF16),
            pltpu.VMEM((width, 2 * width), BF16),
            pltpu.VMEM((bands, rows, 2 * width), BF16),
            pltpu.VMEM((total, rows, 2 * width), BF16),
            pltpu.VMEM((2, bands * rows, width), F32),
            pltpu.VMEM((2, bands * rows, width), F32),
            pltpu.VMEM((4 * bands // fold, bands * fold), F32),
            pltpu.VMEM((reducers, 4 * bands // fold, bands * fold), F32),
            dma((9,)),
            pltpu.SemaphoreType.REGULAR((3,)),
            dma((groups,)),
            dma((groups,)),
            dma((groups,)),
            dma((groups,)),
            dma((per_group,)),
            dma,
            dma((reducers,)),
            dma,
            dma((total,)),
            dma,
        ],
        compiler_params=pltpu.CompilerParams(
            collective_id=0, has_side_effects=True, vmem_limit_bytes=60000000
        ),
    )(orbitals, slot_sticks, stick_entries, potential, tz, tb, tx, ty, tr)
    return pl.pallas_call(
        write_out,
        out_shape=[jax.ShapeDtypeStruct(r.shape, r.dtype) for r in results],
        in_specs=[vmem] * 3,
        out_specs=[hbm] * 3,
        scratch_shapes=[dma((3,))],
    )(*[pltpu.with_memory_space_constraint(r, pltpu.VMEM) for r in results])


def solution(mesh):
    bands = mesh.shape["band"]
    groups = mesh.shape["ga"]
    return jax.shard_map(
        functools.partial(body, bands, groups),
        mesh=mesh,
        in_specs=(P(None, "band", "ga", None), P("ga", None), P(), P()),
        out_specs=(P(None, "band", "ga", None), P(), P()),
        check_vma=False,
    )
```

```python
import functools
import math

import jax
import jax.numpy as jnp
import numpy as np
from jax import lax
from jax.experimental import pallas as pl
from jax.experimental.pallas import tpu as pltpu
from jax.sharding import PartitionSpec as P

MESH = pl.DeviceIdType.MESH
NT = (((1,), (1,)), ((), ()))
BF16 = jnp.bfloat16
F32 = jnp.float32
BLOCK = 4
UNROLL = 8


def split_np(table):
    high = table.astype(np.float32).astype(BF16)
    low = (table - high.astype(np.float64)).astype(np.float32).astype(BF16)
    return np.stack([high, low])


def tables(points, width, radius, groups, planes, plane_pad, coarse):
    freq = np.arange(width) - radius + 1
    used = (np.arange(width) < width - 1).astype(np.float64)
    z_tabs = []
    for group in range(groups):
        z = np.arange(planes) + group * planes
        angle = 2.0 * np.pi * ((freq[:, None] * z[None, :]) % points) / points
        cos = np.zeros((width, plane_pad))
        sin = np.zeros((width, plane_pad))
        cos[:, :planes] = np.cos(angle) * used[:, None]
        sin[:, :planes] = np.sin(angle) * used[:, None]
        z_tabs.append(split_np(np.block([[cos, sin], [-sin, cos]])))
    x = np.arange(coarse)
    angle = 2.0 * np.pi * ((freq[None, :] * x[:, None]) % coarse) / coarse
    cos = np.cos(angle) * used[None, :]
    sin = np.sin(angle) * used[None, :]
    forward = np.block([[cos, -sin], [sin, cos]])
    limit = 2 * (radius - 1)
    offset = (x[:, None] * points - np.arange(points)[None, :] * coarse) % (coarse * points)
    base = 2.0 * np.pi * offset / (coarse * points)
    resample = np.ones((coarse, points))
    for g in range(1, limit + 1):
        resample += 2.0 * np.cos(g * base)
    resample /= points
    z_tabs = np.stack(z_tabs)
    return (
        z_tabs,
        np.swapaxes(z_tabs, 2, 3).copy(),
        split_np(forward),
        split_np(forward.T.copy()),
        split_np(resample),
    )


def split(value):
    high = value.astype(BF16)
    low = (value - high.astype(F32)).astype(BF16)
    return high, low


def thirds(value, axis):
    high, low = split(value)
    return jnp.concatenate([high, low, high], axis=axis)


def dot(a, b):
    return jnp.dot(a, b, preferred_element_type=F32)


def dot_nt(a, b):
    return lax.dot_general(a, b, NT, preferred_element_type=F32)


def take_lanes(value, index):
    return jnp.take_along_axis(value, index, axis=1, mode="promise_in_bounds")


def kernel(
    bands,
    groups,
    points,
    radius,
    orb_hbm,
    slots_hbm,
    entries_hbm,
    pot_hbm,
    tz_hbm,
    tb_hbm,
    tx_hbm,
    ty_hbm,
    tr_hbm,
    out_ref,
    corr_ref,
    red_ref,
    orb_ref,
    slots_ref,
    entries_ref,
    tz,
    tb,
    tx,
    ty,
    tr,
    pot,
    ent_t,
    inv_ref,
    raw,
    spread,
    part,
    got,
    dense_ref,
    pdense,
    inbox_m,
    inbox_p,
    left_f,
    right_f,
    message,
    inbox_s,
    load_sem,
    near_sem,
    s_send,
    s_recv,
    x_send,
    x_recv,
    m_send,
    m_recv,
    p_send,
    p_recv,
    b_send,
    b_recv,
):
    band = lax.axis_index("band")
    ga = lax.axis_index("ga")
    total = bands * groups
    twin = band + 1 - 2 * lax.rem(band, 2)
    me = ga * bands + twin
    slots = orb_hbm.shape[2]
    width = orb_hbm.shape[3]
    planes = pot_hbm.shape[0]
    plane_pad = pot.shape[0]
    coarse = tx.shape[1] // 2
    reducers = inbox_s.shape[0]
    rows = width // reducers
    per_group = reducers // groups
    block = math.gcd(bands, BLOCK)
    blocks = bands // block
    place = lax.rem(band, block)
    base = band - place
    first_band = bands // 2 - per_group + 1

    loads = [
        pltpu.make_async_copy(entries_hbm, entries_ref, load_sem.at[5]),
        pltpu.make_async_copy(orb_hbm, orb_ref, load_sem.at[6]),
        pltpu.make_async_copy(slots_hbm, slots_ref, load_sem.at[7]),
        pltpu.make_async_copy(pot_hbm, pot.at[pl.ds(0, planes)], load_sem.at[0]),
        pltpu.make_async_copy(tr_hbm, tr, load_sem.at[1]),
        pltpu.make_async_copy(tz_hbm.at[ga], tz, load_sem.at[2]),
        pltpu.make_async_copy(tx_hbm, tx, load_sem.at[3]),
        pltpu.make_async_copy(ty_hbm, ty, load_sem.at[4]),
        pltpu.make_async_copy(tb_hbm.at[ga], tb, load_sem.at[8]),
    ]
    load_entries, load_orb, load_slots, load_pot, load_tr, load_tz, load_tx, load_ty, load_tb = loads
    load_orb.start()

    has_low = band >= block
    has_high = band < bands - block
    barrier = pltpu.get_barrier_semaphore()
    across = band + 2 - 4 * lax.rem(lax.div(band, 2), 2)

    def greet(to_band, to_ga, semaphore=barrier):
        pl.semaphore_signal(semaphore, inc=1, device_id=(to_band, to_ga), device_id_type=MESH)

    for k in range(1, groups):
        greet(twin, lax.rem(ga + k, groups))
        greet(band, lax.rem(ga + k, groups))
    greet(twin, ga)
    greet(across, ga)

    def near(semaphore_low, semaphore_high):
        @pl.when(has_low)
        def _():
            pl.semaphore_signal(
                semaphore_high, inc=1, device_id=(band - block, ga), device_id_type=MESH
            )

        @pl.when(has_high)
        def _():
            pl.semaphore_signal(
                semaphore_low, inc=1, device_id=(band + block, ga), device_id_type=MESH
            )

    def near_wait():
        @pl.when(has_low)
        def _():
            pl.semaphore_wait(near_sem.at[0], 1)

        @pl.when(has_high)
        def _():
            pl.semaphore_wait(near_sem.at[1], 1)

    near(barrier, barrier)
    for load in loads:
        if load is not load_orb:
            load.start()
    if plane_pad > planes:
        pot[pl.ds(planes, plane_pad - planes), :] = jnp.zeros(
            (plane_pad - planes, pot.shape[1]), F32
        )

    load_orb.wait()
    pl.semaphore_wait(
        barrier, 2 * groups + has_low.astype(jnp.int32) + has_high.astype(jnp.int32)
    )
    s_copies = []
    for k in range(1, groups + 1):
        for c in range(2):
            copy = pltpu.make_async_remote_copy(
                src_ref=orb_ref.at[c, 0],
                dst_ref=raw.at[ga, c],
                send_sem=s_send.at[k - 1, c],
                recv_sem=s_recv.at[ga, c],
                device_id=(twin, lax.rem(ga + k, groups)),
                device_id_type=MESH,
            )
            copy.start()
            s_copies.append(copy)

    def arrived(ref, sem, g):
        pltpu.make_async_copy(ref.at[g], ref.at[g], sem.at[g]).wait()

    greet(across, ga, near_sem.at[2])

    load_entries.wait()
    load_slots.wait()
    all_slots = groups * slots
    listed = entries_ref[...].astype(F32)
    slot_pad = ent_t.shape[1] - all_slots
    if slot_pad:
        listed = jnp.concatenate([listed, jnp.full((slot_pad, width), -1.0, F32)], axis=0)
    ent_t[...] = listed.T
    lanes = ent_t.shape[1]
    which = lax.broadcasted_iota(jnp.int32, (width, lanes), 0).astype(F32).astype(BF16)

    def invert(step, found):
        for u in range(UNROLL):
            k = step * UNROLL + u
            row = jnp.broadcast_to(ent_t[pl.ds(k, 1), :], (16, lanes)).astype(BF16)
            row = jnp.concatenate([row] * (width // 16), axis=0)
            found = jnp.where(row == which, k.astype(F32).astype(BF16), found)
        return found

    found = lax.fori_loop(
        0, width // UNROLL, invert, jnp.full((width, lanes), -1.0, BF16)
    )
    found = found.astype(F32).T.astype(jnp.int32)
    for g in range(groups):
        inv_ref[g] = found[g * slots : (g + 1) * slots]

    def spread_of(g):
        inverse = inv_ref[g]
        filled = inverse >= 0
        index = jnp.maximum(inverse, 0)
        for c in range(2):
            pltpu.make_async_copy(raw.at[g, c], raw.at[g, c], s_recv.at[g, c]).wait()
            value = take_lanes(raw[g, c].astype(F32), index)
            spread[g, :, c * width : (c + 1) * width] = jnp.where(filled, value, 0.0).astype(BF16)

    re = orb_ref[0, 0].astype(F32)
    im = orb_ref[1, 0].astype(F32)
    spread_of(ga)

    rounds = max(blocks // 2, 1)
    pl.semaphore_wait(near_sem.at[2], 1)
    near(near_sem.at[0], near_sem.at[1])

    load_pot.wait()
    load_tr.wait()
    pot_hi, pot_lo = split(pot[...])
    weight = dot_nt(tr[0], pot_hi) + dot_nt(tr[0], pot_lo) + dot_nt(tr[1], pot_hi)

    near_wait()
    if rounds > 1:
        near(near_sem.at[0], near_sem.at[1])

    all_sticks = slots_ref[...].reshape(1, all_slots)
    sticks = [all_sticks[:, g * slots : (g + 1) * slots] for g in range(groups)]
    sub = lax.broadcasted_iota(jnp.int32, (width, slots), 0)

    def chosen_of(g):
        row = sticks[0]
        for other_ga in range(1, groups):
            row = jnp.where(g == other_ga, sticks[other_ga], row)
        return jnp.where(sub == row, 1.0, 0.0).astype(BF16)

    chosen = [chosen_of(lax.rem(ga + k, groups)) for k in range(1, groups)]
    dense = dot(chosen_of(ga), spread[ga])

    for k in range(1, groups):
        spread_of(lax.rem(ga + k, groups))
    for copy in s_copies:
        copy.wait_send()
    for k in range(1, groups):
        dense += dot(chosen[k - 1], spread[lax.rem(ga + k, groups)])
    dense = dense.astype(BF16)
    dense_ref[...] = dense

    load_tz.wait()
    pair = jnp.concatenate([dense, dense], axis=1)
    z_table = jnp.concatenate([tz[0], tz[1]], axis=0)
    columns = [dot(pair, z_table[:, :plane_pad]), dot(pair, z_table[:, plane_pad:])]
    columns = jnp.concatenate(columns, axis=0)
    load_tx.wait()
    x_table = jnp.concatenate([tx[0], tx[0], tx[1]], axis=1)
    columns = thirds(columns, 0)
    quarter = coarse // 2
    field = jnp.concatenate(
        [dot(x_table[i * quarter : (i + 1) * quarter], columns) for i in range(4)], axis=0
    )
    product = jnp.concatenate([field[:coarse] * weight, field[coarse:] * weight], axis=0)
    product = thirds(product, 0)
    for r in range(1, rounds):
        near_wait()
        if r < rounds - 1:
            near(near_sem.at[0], near_sem.at[1])

    def place_of(r):
        return first_band + 2 * lax.rem(r, per_group), lax.div(r, per_group)

    def other(to_band, to_ga):
        own = (to_band == band) & (to_ga == ga)
        return jnp.where(own, band - 1, to_band), to_ga

    m_copies = []
    for q in range(per_group):
        start = pl.multiple_of((ga * per_group + q) * rows, rows)
        m_copies.append(
            pltpu.make_async_remote_copy(
                src_ref=dense_ref.at[pl.ds(start, rows)],
                dst_ref=inbox_m.at[twin],
                send_sem=m_send.at[q],
                recv_sem=m_recv,
                device_id=other(first_band + 2 * q, ga),
                device_id_type=MESH,
            )
        )
        m_copies[-1].start()

    load_ty.wait()
    y_table = jnp.concatenate([ty[0], ty[0], ty[1]], axis=1)
    back = jnp.concatenate([dot(y_table[:width], product), dot(y_table[width:], product)], axis=0)
    back = thirds(jnp.concatenate([back[:width], back[width:]], axis=1), 1)
    load_tb.wait()
    spectra = dot(back, jnp.concatenate([tb[0], tb[0], tb[1]], axis=0))
    spectra = spectra * (1.0 / float(points * coarse))
    spec_hi, spec_lo = split(spectra)
    pdense[...] = spec_hi

    nearest = jnp.where(
        band >= bands // 2, per_group // 2 + lax.div(lax.rem(band, block), 2), lax.div(lax.rem(band, block), 2)
    )
    nearest = lax.rem(nearest, per_group)

    def far_reducer(far):
        g = lax.rem(ga + far // per_group, groups)
        q, bit = 0, 1
        while bit < per_group:
            own_bit = lax.rem(lax.div(nearest, bit), 2)
            q = q + bit * (1 - own_bit if far % per_group & bit else own_bit)
            bit *= 2
        return g * per_group + q

    p_copies = []
    for far in reversed(range(reducers)):
        r = far_reducer(far)
        p_copies.append(
            pltpu.make_async_remote_copy(
                src_ref=pdense.at[pl.ds(pl.multiple_of(r * rows, rows), rows)],
                dst_ref=inbox_p.at[me],
                send_sem=p_send.at[far],
                recv_sem=p_recv,
                device_id=other(*place_of(r)),
                device_id_type=MESH,
            )
        )
        p_copies[-1].start()

    eye = lax.broadcasted_iota(jnp.int32, (slots, slots), 0) == lax.broadcasted_iota(
        jnp.int32, (slots, slots), 1
    )

    def stick_column(g):
        row = sticks[0]
        for other in range(1, groups):
            row = jnp.where(g == other, sticks[other], row)
        row = row.astype(F32)
        return jnp.sum(jnp.where(eye, row, 0.0), axis=1, keepdims=True)

    lane = lax.broadcasted_iota(jnp.int32, (slots, width), 1)
    lane_f = lane.astype(F32)
    x_copies = []
    for k in range(1, groups + 1):
        target = lax.rem(ga + k, groups)
        stick = stick_column(target)
        choose = jnp.where(stick == lane_f, 1.0, 0.0).astype(BF16)
        mine = dot(choose, spec_hi) + dot(choose, spec_lo)
        part[k - 1] = mine
        x_copies.append(
            pltpu.make_async_remote_copy(
                src_ref=part.at[k - 1],
                dst_ref=got.at[ga],
                send_sem=x_send.at[k - 1],
                recv_sem=x_recv.at[ga],
                device_id=(twin, target),
                device_id_type=MESH,
            )
        )

    own = entries_ref[pl.ds(pl.multiple_of(ga * slots, 8), slots)]
    present = own >= 0
    gx = stick - float(radius - 1)
    gz = (own - (radius - 1)).astype(F32)
    kinetic = (gx * gx + gz * gz) * (1.0 / float(radius * radius))
    own_index = jnp.maximum(own, 0)

    for copy in x_copies:
        copy.start()

    offset = band - first_band
    is_reducer = (offset >= 0) & (offset < 2 * per_group) & (lax.rem(band + 1, 2) == 0)
    number = ga * per_group + lax.div(jnp.clip(offset, 0, 2 * per_group - 1), 2)

    order = band * groups + ga

    def b_copy(t):
        if isinstance(t, int):
            to_band, to_ga = t // groups, t % groups
        else:
            to_band, to_ga = lax.div(t, groups), lax.rem(t, groups)
        return pltpu.make_async_remote_copy(
            src_ref=message,
            dst_ref=inbox_s.at[number],
            send_sem=b_send.at[t],
            recv_sem=b_recv,
            device_id=(to_band, to_ga),
            device_id_type=MESH,
        )

    def b_each(act):
        if total <= 64:
            for t in range(total):

                @pl.when(order != t)
                def _(t=t):
                    act(b_copy(t))
        else:

            @pl.loop(0, total)
            def _(t):
                @pl.when(order != t)
                def _():
                    act(b_copy(t))

    def keep(ref, value):
        for c in range(2):
            ref[c] = value[:, :, c * width : (c + 1) * width].reshape(bands * rows, width)

    @pl.when(is_reducer)
    def _():
        m_all = inbox_m.at[pl.ds(0, bands - 1)]
        pltpu.make_async_copy(m_all, m_all, m_recv).wait()
        own_rows = pl.ds(pl.multiple_of(number * rows, rows), rows)
        inbox_m[twin] = dense_ref[own_rows, :]
        inbox_p[me] = pdense[own_rows, :]
        left = inbox_m[...].astype(F32)
        row_id = lax.broadcasted_iota(jnp.int32, (rows, 2 * width), 0) + number * rows
        lane_id = lax.broadcasted_iota(jnp.int32, (rows, 2 * width), 1)
        row_f = (row_id - (radius - 1)).astype(F32)
        lane_g = (jnp.where(lane_id >= width, lane_id - width, lane_id) - (radius - 1)).astype(F32)
        kin = (row_f * row_f + lane_g * lane_g) * (1.0 / float(radius * radius))
        right = left * kin[None]
        keep(left_f, left)

        def overlaps(source):
            result = jnp.zeros((2 * bands, bands), F32)
            for r in range(rows):
                every = pl.ds(r, bands, stride=rows)
                low = jnp.concatenate([left_f[0, every, :], left_f[1, every, :]], axis=1)
                high_re, high_im = source[0, every, :], source[1, every, :]
                stack = jnp.concatenate(
                    [
                        jnp.concatenate([high_re, high_im], axis=1),
                        jnp.concatenate([-high_im, high_re], axis=1),
                    ],
                    axis=0,
                )
                result += dot_nt(stack.astype(BF16), low.astype(BF16))
            return result * (1.0 / float(4 * radius * radius))

        corr = overlaps(left_f)
        p_all = inbox_p.at[pl.ds(0, total - 1)]
        pltpu.make_async_copy(p_all, p_all, p_recv).wait()
        for g in range(groups):
            right += inbox_p[g * bands : (g + 1) * bands].astype(F32)
        keep(right_f, right)
        result = jnp.concatenate([overlaps(right_f), corr], axis=0)
        depth = message.shape[0]
        message[...] = jnp.concatenate(
            [result[f : f + depth] for f in range(0, 4 * bands, depth)], axis=1
        )
        inbox_s[number] = message[...]
        b_each(lambda copy: copy.start())

    for g in range(groups):
        arrived(got, x_recv, g)
    mine = got[0]
    for g in range(1, groups):
        mine += got[g]
    a_re = take_lanes(mine[:, :width], own_index)
    a_im = take_lanes(mine[:, width:], own_index)
    out_ref[0, 0] = jnp.where(present, kinetic * re + a_re, 0.0).astype(BF16)
    out_ref[1, 0] = jnp.where(present, kinetic * im + a_im, 0.0).astype(BF16)

    for copy in m_copies + p_copies + x_copies:
        copy.wait_send()

    @pl.when(is_reducer)
    def _():
        most = inbox_s.at[pl.ds(0, reducers - 1)]
        pltpu.make_async_copy(most, most, b_recv).wait()

    beside = (offset + 1 >= 0) & (offset + 1 < 2 * per_group) & (lax.rem(band, 2) == 0)

    @pl.when(beside)
    def _():
        pltpu.make_async_copy(inbox_m.at[0], inbox_m.at[0], m_recv).wait()
        pltpu.make_async_copy(inbox_p.at[0], inbox_p.at[0], p_recv).wait()

    @pl.when(jnp.logical_not(is_reducer))
    def _():
        pltpu.make_async_copy(inbox_s, inbox_s, b_recv).wait()

    final = inbox_s[0]
    for r in range(1, reducers):
        final += inbox_s[r]
    final = jnp.concatenate(
        [final[:, f : f + bands] for f in range(0, final.shape[1], bands)], axis=0
    )
    red_ref[0] = final[:bands]
    red_ref[1] = final[bands : 2 * bands]
    corr_ref[0] = final[2 * bands : 3 * bands]
    corr_ref[1] = final[3 * bands :]


    @pl.when(is_reducer)
    def _():
        b_each(lambda copy: copy.wait_send())


def write_out(out_ref, corr_ref, red_ref, out_hbm, corr_hbm, red_hbm, sem):
    copies = [
        pltpu.make_async_copy(out_ref, out_hbm, sem.at[0]),
        pltpu.make_async_copy(corr_ref, corr_hbm, sem.at[1]),
        pltpu.make_async_copy(red_ref, red_hbm, sem.at[2]),
    ]
    for copy in copies:
        copy.start()
    for copy in copies:
        copy.wait()


def body(bands, groups, orbitals, potential, slot_sticks, stick_entries):
    points = potential.shape[1]
    planes = potential.shape[0]
    width = stick_entries.shape[1]
    radius = width // 2
    slots = orbitals.shape[2]
    plane_pad = -(-planes // 128) * 128
    coarse = 2 * width
    reducers = width // 16
    per_group = reducers // groups
    rows = width // reducers
    fold = max(1, 128 // bands)
    slot_lanes = -(-groups * slots // 128) * 128
    tz, tb, tx, ty, tr = tables(points, width, radius, groups, planes, plane_pad, coarse)
    vmem = pl.BlockSpec(memory_space=pltpu.VMEM)
    hbm = pl.BlockSpec(memory_space=pltpu.HBM)
    total = bands * groups
    dma = pltpu.SemaphoreType.DMA
    results = pl.pallas_call(
        functools.partial(kernel, bands, groups, points, radius),
        out_shape=(
            pltpu.VMEM(orbitals.shape, BF16),
            pltpu.VMEM((2, bands, bands), F32),
            pltpu.VMEM((2, bands, bands), F32),
        ),
        in_specs=[hbm] * 9,
        out_specs=(vmem, vmem, vmem),
        scratch_shapes=[
            pltpu.VMEM(orbitals.shape, BF16),
            pltpu.VMEM(slot_sticks.shape, jnp.int32),
            pltpu.VMEM(stick_entries.shape, jnp.int32),
            pltpu.VMEM(tz.shape[1:], BF16),
            pltpu.VMEM(tb.shape[1:], BF16),
            pltpu.VMEM(tx.shape, BF16),
            pltpu.VMEM(ty.shape, BF16),
            pltpu.VMEM(tr.shape, BF16),
            pltpu.VMEM((plane_pad, points), F32),
            pltpu.VMEM((width, slot_lanes), F32),
            pltpu.VMEM((groups, slots, width), jnp.int32),
            pltpu.VMEM((groups, 2, slots, width), BF16),
            pltpu.VMEM((groups, slots, 2 * width), BF16),
            pltpu.VMEM((groups, slots, 2 * width), F32),
            pltpu.VMEM((groups, slots, 2 * width), F32),
            pltpu.VMEM((width, 2 * width), BF16),
            pltpu.VMEM((width, 2 * width), BF16),
            pltpu.VMEM((bands, rows, 2 * width), BF16),
            pltpu.VMEM((total, rows, 2 * width), BF16),
            pltpu.VMEM((2, bands * rows, width), F32),
            pltpu.VMEM((2, bands * rows, width), F32),
            pltpu.VMEM((4 * bands // fold, bands * fold), F32),
            pltpu.VMEM((reducers, 4 * bands // fold, bands * fold), F32),
            dma((9,)),
            pltpu.SemaphoreType.REGULAR((3,)),
            dma((groups, 2)),
            dma((groups, 2)),
            dma((groups,)),
            dma((groups,)),
            dma((per_group,)),
            dma,
            dma((reducers,)),
            dma,
            dma((total,)),
            dma,
        ],
        compiler_params=pltpu.CompilerParams(
            collective_id=0, has_side_effects=True, vmem_limit_bytes=60000000
        ),
    )(orbitals, slot_sticks, stick_entries, potential, tz, tb, tx, ty, tr)
    return pl.pallas_call(
        write_out,
        out_shape=[jax.ShapeDtypeStruct(r.shape, r.dtype) for r in results],
        in_specs=[vmem] * 3,
        out_specs=[hbm] * 3,
        scratch_shapes=[dma((3,))],
    )(*[pltpu.with_memory_space_constraint(r, pltpu.VMEM) for r in results])


def solution(mesh):
    bands = mesh.shape["band"]
    groups = mesh.shape["ga"]
    return jax.shard_map(
        functools.partial(body, bands, groups),
        mesh=mesh,
        in_specs=(P(None, "band", "ga", None), P("ga", None), P(), P()),
        out_specs=(P(None, "band", "ga", None), P(), P()),
        check_vma=False,
    )
```
